512 devices in a mesh: paths: 32 (over x, z), trades: 16 (over y, core).
Axes of the slice: x: 4, y: 8, z: 8, core: 2. Of those that a mesh axis runs over, the one named last changes fastest.
Arguments:
- x_train: float32 [8192, 64], P('paths'), may hold values from -6 to 6
- value_label: float32 [8192, 4096], P('paths', 'trades'), may hold values from -6 to 6
- slope_label: float32 [8192, 64], P('paths'), may hold values from -6 to 6
- x_infer: float32 [4, 8192, 64], P(None, 'paths'), may hold values from -6 to 6
- w_in: float32 [64, 512], replicated, may hold values from -0.75 to 0.75
- b_in: float32 [512], replicated, may hold values from -3 to 3
- w_mid: float32 [512, 512], replicated, may hold values from -0.25 to 0.25
- b_mid: float32 [512], replicated, may hold values from -3 to 3
- head: float32 [512, 4096], P(None, 'trades'), may hold values from -0.25 to 0.25
- trade_set: int32 [4096], P('trades'), may hold values from 0 to 255
- trade_sign: int32 [4096], P('trades'), may hold values from 0 to 1
- trade_level: int32 [4096], P('trades'), may hold values from 0 to 7
Outputs:
- grad_w_in: float32 [64, 512], replicated
- grad_b_in: float32 [512], replicated
- grad_w_mid: float32 [512, 512], replicated
- grad_b_mid: float32 [512], replicated
- grad_head: float32 [512, 4096], P(None, 'trades')
- exposure: float32 [4, 256], P(None, 'trades')
The draws below stay inside these ranges and needn't reach their ends.
All inputs are finite; a program needn't handle non-finite values.
Results may differ from the reference program's by a relative error of at most 0.000061.
Values sent between devices are 32-bit elements; how exact they have to be, the bound alone decides.
No kernel may reach another device: no remote copies, remote signals or barrier semaphores. Data moves between devices by JAX's collectives and lax.ppermute only.
A program may use at most 64 MiB of HBM per device.

```python
import math
import jax
import jax.numpy as jnp
from jax import lax

FACT = 64
HID = 512
TRADES = 4096
SETS = 256
DATES = 4
PATH_DEV = 256
TRAIN = 8192
INFER = 8192


def block_offsets(key, row_count, column_count):
    block_count = row_count // PATH_DEV
    subkeys = jax.random.split(key, 6)
    block_index = jnp.arange(block_count, dtype=jnp.int32)
    half_sign = jnp.where(block_index < block_count // 2, 1.0, -1.0).astype(jnp.float32)
    quarter = block_count // 4
    inner = (block_index >= quarter) & (block_index < block_count - quarter)
    middle_sign = jnp.where(inner, 1.0, -1.0).astype(jnp.float32)
    first_scale = jax.random.uniform(subkeys[0], (block_count,), jnp.float32, 0.8, 1.3)
    second_scale = jax.random.uniform(subkeys[1], (block_count,), jnp.float32, 0.8, 1.3)
    noise_part = jax.random.normal(subkeys[5], (row_count, column_count), jnp.float32)
    first_pattern = jax.random.normal(subkeys[2], (column_count,), jnp.float32)
    second_pattern = jax.random.normal(subkeys[3], (column_count,), jnp.float32)
    block_level = (half_sign * first_scale)[:, None] * first_pattern[None, :] + (middle_sign * second_scale)[:, None] * second_pattern[None, :]
    row_level = jnp.repeat(block_level, PATH_DEV, axis=0)
    return jnp.clip(noise_part + row_level, -6.0, 6.0)


def draw_value_label(key, part):
    return block_offsets(jax.random.fold_in(key, 101), TRAIN, TRADES)


def draw_slope_label(key, part):
    return block_offsets(jax.random.fold_in(key, 202), TRAIN, FACT)


def set_ends(result, key, smallest, largest):
    index_at = [jax.random.randint(jax.random.fold_in(key, axis), (), 0, length) for axis, length in enumerate(result.shape)]
    main_axis = result.shape.index(max(result.shape))
    next_to = index_at[:main_axis] + [(index_at[main_axis] + 1) % result.shape[main_axis]] + index_at[main_axis + 1:]
    return result.at[tuple(index_at)].set(smallest).at[tuple(next_to)].set(largest)


def block_scale(key, shape, cuts, least, high):
    loudness = 1.0
    for dim, parts in cuts:
        steps = jax.random.uniform(jax.random.fold_in(jax.random.fold_in(key, 6), dim), (parts,), jnp.float32, least / len(cuts), high / len(cuts))
        loudness = loudness * jnp.repeat(jnp.exp(steps), shape[dim] // parts).reshape((-1,) + (1,) * (len(shape) - 1 - dim))
    return loudness


def gaussian(own_key, shape, deviation, reach, cuts=(), kind=jnp.bfloat16):
    loudness = block_scale(own_key, shape, cuts, -0.22, 0.18) if cuts else 1.0
    entries = jax.random.normal(own_key, shape, jnp.float32) * deviation * loudness
    return jnp.minimum(jnp.maximum(entries, -reach), reach).astype(kind)


def setup_inputs(seed: int = 0) -> dict:
    splits = jax.random.split(jax.random.key(seed), 13)
    return {
        "x_train": gaussian(splits[0], (TRAIN, FACT), 1.0, 6.0, ((0, 32),), jnp.float32),
        "value_label": draw_value_label(jax.random.fold_in(splits[12], 71), 0),
        "slope_label": draw_slope_label(jax.random.fold_in(splits[12], 71), 0),
        "x_infer": gaussian(splits[3], (DATES, INFER, FACT), 1.0, 6.0, ((1, 32),), jnp.float32),
        "w_in": gaussian(splits[4], (FACT, HID), FACT ** -0.5, 0.75, (), jnp.float32),
        "b_in": gaussian(splits[5], (HID,), 0.5, 3.0, (), jnp.float32),
        "w_mid": gaussian(splits[6], (HID, HID), HID ** -0.5, 0.25, (), jnp.float32),
        "b_mid": gaussian(splits[7], (HID,), 0.5, 3.0, (), jnp.float32),
        "head": gaussian(splits[8], (HID, TRADES), HID ** -0.5, 0.25, ((1, 16),), jnp.float32),
        "trade_set": set_ends(jax.random.randint(splits[9], (TRADES,), 0, SETS), jax.random.fold_in(splits[9], 1), 0, SETS - 1).astype(jnp.int32),
        "trade_sign": set_ends(jax.random.randint(splits[10], (TRADES,), 0, 2), jax.random.fold_in(splits[10], 1), 0, 1).astype(jnp.int32),
        "trade_level": set_ends(jax.random.randint(splits[11], (TRADES,), 0, 8), jax.random.fold_in(splits[11], 1), 0, 7).astype(jnp.int32),
    }


learn_rate = 0.5

def mat_mul(left, right):
    return jnp.dot(left, right, precision=lax.Precision.HIGHEST, preferred_element_type=jnp.float32)

def trade_weights(trade_sign, trade_level):
    return (2 * trade_sign - 1).astype(jnp.float32) * (0.5 + 0.25 * trade_level.astype(jnp.float32))

def trunk_slope(inputs, w_in, b_in, w_mid, b_mid, portfolio):
    first_pre = mat_mul(inputs, w_in) + b_in
    first_act = jax.nn.softplus(first_pre)
    second_pre = mat_mul(first_act, w_mid) + b_mid
    second_act = jax.nn.softplus(second_pre)
    back_mid = portfolio * jax.nn.sigmoid(second_pre)
    back_first = mat_mul(back_mid, w_mid.T) * jax.nn.sigmoid(first_pre)
    return (second_act, mat_mul(back_first, w_in.T))

def features(inputs, w_in, b_in, w_mid, b_mid):
    first_act = jax.nn.softplus(mat_mul(inputs, w_in) + b_in)
    return jax.nn.softplus(mat_mul(first_act, w_mid) + b_mid)

def reference(x_train, value_label, slope_label, x_infer, w_in, b_in, w_mid, b_mid, head, trade_set, trade_sign, trade_level):
    weights = trade_weights(trade_sign, trade_level)
    scale = 1.0 / math.sqrt(TRADES)

    def loss(params):
        p_in, q_in, p_mid, q_mid, p_head = params
        portfolio = mat_mul(p_head, weights) * scale
        second_act, slopes = trunk_slope(x_train, p_in, q_in, p_mid, q_mid, portfolio)
        values = mat_mul(second_act, p_head)
        value_err = values - value_label
        slope_err = slopes - slope_label
        return jnp.sum(value_err * value_err) / (TRAIN * TRADES) + jnp.sum(slope_err * slope_err) / (TRAIN * FACT)
    params = (w_in, b_in, w_mid, b_mid, head)
    grads = jax.grad(loss)(params)
    updated = tuple((p - learn_rate * g for p, g in zip(params, grads)))
    member = (trade_set[:, None] == jnp.arange(SETS, dtype=jnp.int32)[None, :]).astype(jnp.float32) * weights[:, None]

    def one_date(inputs):
        act = features(inputs, updated[0], updated[1], updated[2], updated[3])
        values = mat_mul(act, updated[4])
        netted = mat_mul(values, member)
        return lax.optimization_barrier(jnp.sum(jnp.maximum(netted, 0.0), axis=0)) / INFER
    exposure = lax.map(one_date, x_infer)
    return (grads[0], grads[1], grads[2], grads[3], grads[4], exposure)
```

```python
import functools

import jax
import jax.numpy as jnp
from jax import lax
from jax.experimental import pallas as pl
from jax.experimental.pallas import tpu as pltpu
from jax.sharding import Mesh
from jax.sharding import PartitionSpec as P

TRADES = ("trades_0", "trades_1")
F32 = jnp.float32
BF16 = jnp.bfloat16

NN = (((1,), (0,)), ((), ()))
NT = (((1,), (1,)), ((), ()))

VALUE_SCALE = 2.0 / (8192 * 4096)
SLOPE_SCALE = 2.0 / (8192 * 64)
PORT_SCALE = 1.0 / 64.0
LEARN = 0.5

LANE_BMID = 96
LANE_BIN = 104
LANE_PORT = 105
LANE_NET = 112


def halves(a):
    high = a.astype(BF16)
    low = (a - high.astype(F32)).astype(BF16)
    return high, low


def mm(left, right, dims=NN):
    def dot(a, b):
        return lax.dot_general(a, b, dims, preferred_element_type=F32)

    return dot(left[0], right[0]) + (dot(left[0], right[1]) + dot(left[1], right[0]))


def softplus_sigmoid(z):
    e = jnp.exp(-jnp.abs(z))
    act = jnp.maximum(z, 0.0) + jnp.log1p(e)
    slope = jnp.where(z >= 0, 1.0, e) / (1.0 + e)
    return act, slope


def softplus(z):
    return jnp.maximum(z, 0.0) + jnp.log1p(jnp.exp(-jnp.abs(z)))


def trade_weights(sign, level):
    return (2 * sign - 1).astype(F32) * (0.5 + 0.25 * level.astype(F32))


def column_of(row):
    return jnp.broadcast_to(row, (128, row.shape[1])).T[:, 0:1]


def lane_index(shape):
    return lax.broadcasted_iota(jnp.int32, shape, len(shape) - 1)


def forward_kernel(
    x, w_in, b_in, w_mid, b_mid, head, label, sign, level,
    pay, a1_t, s1_t, s2_t, a2_t, dv_t, w_in_t, w_mid_t,
):
    wt = w_in[...].T
    w_in_t[...] = wt
    z1 = mm(halves(wt), halves(x[...]), NT) + column_of(b_in[...])
    a1, s1 = softplus_sigmoid(z1)
    a1_t[...] = a1
    s1_t[...] = s1
    mt = w_mid[...].T
    w_mid_t[...] = mt
    z2 = mm(halves(mt), halves(a1)) + column_of(b_mid[...])
    a2, s2 = softplus_sigmoid(z2)
    a2_t[...] = a2
    s2_t[...] = s2
    hd = head[...]
    hp = halves(hd)
    values = mm(halves(hd.T), halves(a2))
    err = (values - label[...].T) * VALUE_SCALE
    dv_t[...] = err
    d_a2 = mm(hp, halves(err))
    pay[:, 0:32, :] = d_a2[:, 0:128].reshape(16, 32, 128)
    pay[:, 32:64, :] = d_a2[:, 128:256].reshape(16, 32, 128)
    w = trade_weights(sign[...], level[...])
    port = jnp.sum(hd * w, axis=1, keepdims=True)
    for k in range(4):
        col = jnp.broadcast_to(port[128 * k : 128 * k + 128], (128, 128))
        row = col.T[0:1]
        pay[:, 64 + k : 65 + k, :] = jnp.broadcast_to(row[None], (16, 1, 128))
    pay[:, 68:72, :] = jnp.zeros((16, 4, 128), F32)


def head_grad_kernel(a2_t, dv_t, out):
    out[...] = mm(halves(a2_t[...]), halves(dv_t[...]), NT)


def backward_kernel(
    own, arrived, x, slope_label_t, w_in, w_in_t, w_mid, w_mid_t, a1_t, s1_t, s2_t, g_head,
    pay, u2_s, q_s, z_s,
):
    rows = pl.ds(pl.multiple_of(own[0] * 32, 32), 32)
    total = jnp.sum(arrived[...], axis=0)
    d_a2 = jnp.concatenate([total[0:32], total[32:64]], axis=1)
    port = jnp.concatenate(
        [column_of(total[64 + k : 65 + k]) for k in range(4)], axis=0
    ) * PORT_SCALE
    s1 = s1_t[...]
    s2 = s2_t[...]
    u2 = port * s2
    u2_s[...] = u2
    v1 = mm(halves(w_mid[...]), halves(u2))
    u1 = v1 * s1
    slopes = mm(halves(w_in[...]), halves(u1))
    d_slope = (slopes - slope_label_t[...]) * SLOPE_SCALE
    du1 = mm(halves(w_in_t[...]), halves(d_slope))
    dv1 = du1 * s1
    ds1 = du1 * v1
    dv1_p = halves(dv1)
    du2 = mm(halves(w_mid_t[...]), dv1_p)
    du2_s2 = du2 * s2
    g_port = jnp.sum(du2_s2, axis=1, keepdims=True)
    q_s[...] = du2_s2 * port * (1.0 - s2)
    dz2 = d_a2 * s2_t[rows, :] + q_s[rows, :]
    z_s[...] = jnp.zeros_like(z_s)
    z_s[rows, :] = dz2
    da1 = mm(halves(w_mid[...]), halves(z_s[...]))
    dz1 = da1 * s1 + (ds1 * s1 * (1.0 - s1)) * (1.0 / 16.0)
    g_b_in = jnp.sum(dz1, axis=1, keepdims=True)
    none = jnp.zeros((64, 256), F32)
    few = jnp.zeros((32, 256), F32)
    mid_a = jnp.concatenate([none, dz2, few], axis=0)
    mid_b = jnp.concatenate([none, u2_s[rows, :], few], axis=0)
    slope_rows = jnp.concatenate([d_slope * (1.0 / 16.0), none], axis=0)
    x_t = jnp.concatenate([x[...].T, none], axis=0)
    ext = mm(halves(a1_t[...]), halves(mid_a), NT)
    ext = ext + mm(dv1_p, halves(mid_b), NT)
    ext = ext + mm(halves(u1), halves(slope_rows), NT)
    ext = ext + mm(halves(dz1), halves(x_t), NT)
    lane = lane_index((512, 128))
    ext = jnp.where(lane == LANE_BIN, g_b_in, ext)
    ext = jnp.where(lane == LANE_PORT, g_port, ext)
    b_mid = jnp.sum(dz2, axis=1, keepdims=True)
    unit = lax.broadcasted_iota(jnp.int32, (32, 128), 0)
    spot = lane_index((32, 128)) == LANE_BMID + (unit & 7)
    spread = jnp.where(spot, b_mid, 0.0)
    lines = [jnp.sum(spread[8 * k : 8 * k + 8], axis=0, keepdims=True) for k in range(4)]
    tile = jnp.concatenate(lines + [jnp.zeros((4, 128), F32)], axis=0)
    blocks = ext.reshape(64, 8, 128) + tile[None]
    pay[:, 0:8, :] = blocks[0:32]
    pay[:, 8:16, :] = blocks[32:64]
    pay[:, 16:24, :] = g_head[0:256, 0:128].reshape(32, 8, 128)
    pay[:, 24:32, :] = g_head[0:256, 128:256].reshape(32, 8, 128)
    pay[:, 32:40, :] = g_head[256:512, 0:128].reshape(32, 8, 128)
    pay[:, 40:48, :] = g_head[256:512, 128:256].reshape(32, 8, 128)


def net_kernel(own, arrived, head, sets, sign, level, pay, head_shard):
    total = jnp.sum(arrived[...], axis=0)
    trunk = total[0:16]
    w = trade_weights(sign[...], level[...])
    upper = jnp.concatenate([total[16:24], total[24:32]], axis=1)
    lower = jnp.concatenate([total[32:40], total[40:48]], axis=1)
    g_head = jnp.concatenate([upper, lower], axis=0)
    g_head = g_head + trunk[:, LANE_PORT : LANE_PORT + 1] * (w * PORT_SCALE)
    head_shard[0:8, :] = g_head[0:8, 0:128]
    head_shard[8:16, :] = g_head[0:8, 128:256]
    head_shard[16:24, :] = g_head[8:16, 0:128]
    head_shard[24:32, :] = g_head[8:16, 128:256]
    first = pl.multiple_of(own[0] * 8, 8)
    second = pl.multiple_of(own[0] * 8 + 256, 8)
    old = jnp.concatenate([head[pl.ds(first, 8), :], head[pl.ds(second, 8), :]], axis=0)
    weighted = halves((old - LEARN * g_head) * w)
    ids = jnp.broadcast_to(sets[...], (128, 256))
    place = lax.broadcasted_iota(jnp.int32, (128, 256), 0) - LANE_NET
    lane = lane_index((16, 128))
    for t in range(16):
        member = ((ids == place + 16 * t) & (place >= 0)).astype(F32).astype(BF16)
        net = lax.dot_general(weighted[0], member, NT, preferred_element_type=F32)
        net = net + lax.dot_general(weighted[1], member, NT, preferred_element_type=F32)
        pay[t] = jnp.where(lane < LANE_NET, trunk, net)


def gather_kernel(core, arrived, pay, g_b_mid):
    total = jnp.sum(arrived[...], axis=0)
    lane = lane_index((16, 128))
    row_lane = lane_index((1, 128))
    first = core[0] == 0
    tiles = []
    for k in range(4):
        block = jnp.zeros((16, 128), F32)
        bias = jnp.zeros((1, 128), F32)
        for m in range(4):
            part = arrived[4 * k + m]
            moved = part if m == 2 else pltpu.roll(part, (32 * m - 64) % 128, 1)
            block = jnp.where((lane >= 32 * m) & (lane < 32 * m + 32), moved, block)
            for r in range(4):
                to = 32 * m + 8 * r
                shift = (to - LANE_BMID) % 128
                line = part[0:8] if shift == 0 else pltpu.roll(part[0:8], shift, 1)
                bias = jnp.where((row_lane >= to) & (row_lane < to + 8), line[r : r + 1], bias)
        g_b_mid[:, 128 * k : 128 * k + 128] = bias
        tiles.append(jnp.where(first, block[0:8], block[8:16]))
    packed = jnp.concatenate(tiles + [total], axis=0)
    pay[...] = jnp.broadcast_to(packed[None], (32, 48, 128))


def infer_kernel(
    core, mine, other, w_in, b_in, w_mid, b_mid, g_b_mid, x, head_shard,
    g_in_out, g_b_in_out, g_mid_out, pay,
):
    first = core[0] == 0
    for k in range(4):
        a = mine[:, 8 * k : 8 * k + 8, :].reshape(256, 128)
        b = other[:, 8 * k : 8 * k + 8, :].reshape(256, 128)
        g_mid_out[0:256, 128 * k : 128 * k + 128] = jnp.where(first, a, b)
        g_mid_out[256:512, 128 * k : 128 * k + 128] = jnp.where(first, b, a)
    upper = mine[:, 32:40, :].reshape(256, 128)
    lower = mine[:, 40:48, :].reshape(256, 128)
    both = jnp.concatenate([upper, lower], axis=0)
    flat = both.T
    g_in = flat[0:64]
    g_b_in = flat[LANE_BIN : LANE_BIN + 1]
    g_in_out[...] = g_in
    g_b_in_out[...] = g_b_in
    new_in = halves(w_in[...] - LEARN * g_in)
    new_b_in = b_in[...] - LEARN * g_b_in
    new_mid = halves(w_mid[...] - LEARN * g_mid_out[...])
    new_b_mid = b_mid[...] - LEARN * g_b_mid[...]
    net_head = halves(both)
    sums = []
    for d in range(4):
        a1 = softplus(mm(halves(x[d]), new_in) + new_b_in)
        a2 = softplus(mm(halves(a1), new_mid) + new_b_mid)
        netted = mm(halves(a2), net_head)
        sums.append(jnp.sum(jnp.maximum(netted, 0.0), axis=0, keepdims=True))
    tile = jnp.concatenate(sums + [jnp.zeros((4, 128), F32)], axis=0)
    pay[:, 0:32, :] = jnp.broadcast_to(head_shard[...][None], (32, 32, 128))
    pay[:, 32:40, :] = jnp.broadcast_to(tile[None], (32, 8, 128))


def finish_kernel(arrived, g_head, exposure):
    g_head[0:256, 0:128] = arrived[:, 0:8, :].reshape(256, 128)
    g_head[0:256, 128:256] = arrived[:, 8:16, :].reshape(256, 128)
    g_head[256:512, 0:128] = arrived[:, 16:24, :].reshape(256, 128)
    g_head[256:512, 128:256] = arrived[:, 24:32, :].reshape(256, 128)
    total = jnp.sum(arrived[:, 32:40, :], axis=0) * (1.0 / 8192.0)
    moved = pltpu.roll(total, 128 - LANE_NET, 1)
    exposure[...] = moved[0:4, 0:16]


def call(kernel, outs, scalars, args, scratch=(), flops=0):
    shapes = tuple(jax.ShapeDtypeStruct(s, F32) for s in outs)
    vmem = pl.BlockSpec(memory_space=pltpu.VMEM)
    smem = pl.BlockSpec(memory_space=pltpu.SMEM)
    return pl.pallas_call(
        kernel,
        out_shape=shapes,
        in_specs=[smem] * len(scalars) + [vmem] * len(args),
        out_specs=tuple(vmem for _ in outs),
        scratch_shapes=[pltpu.VMEM(s, F32) for s in scratch],
        cost_estimate=pl.CostEstimate(flops=flops, transcendentals=0, bytes_accessed=0),
        name=kernel.__name__,
    )(*scalars, *args)


def swap(x, axis):
    return lax.all_to_all(x, axis, 0, 0, tiled=True)


def on_device(
    x_train, value_label, slope_label, x_infer, w_in, b_in, w_mid, b_mid, head,
    trade_set, trade_sign, trade_level,
):
    path = lax.axis_index("paths").astype(jnp.int32).reshape(1)
    trade = lax.axis_index(TRADES).astype(jnp.int32).reshape(1)
    core = lax.axis_index("trades_1").astype(jnp.int32).reshape(1)
    b_in_r = b_in.reshape(1, -1)
    b_mid_r = b_mid.reshape(1, -1)
    sets = trade_set.reshape(1, -1)
    sign = trade_sign.reshape(1, -1)
    level = trade_level.reshape(1, -1)
    act = (512, 256)
    pay1, a1_t, s1_t, s2_t, a2_t, dv_t, w_in_t, w_mid_t = call(
        forward_kernel,
        [(16, 72, 128), act, act, act, act, (256, 256), (512, 64), (512, 512)],
        [],
        [x_train, w_in, b_in_r, w_mid, b_mid_r, head, value_label, sign, level],
        flops=10**9,
    )
    arr1 = swap(pay1, TRADES)
    (g_head,) = call(head_grad_kernel, [act], [], [a2_t, dv_t], flops=4 * 10**8)
    (pay2,) = call(
        backward_kernel,
        [(32, 48, 128)],
        [trade],
        [arr1, x_train, slope_label.T, w_in, w_in_t, w_mid, w_mid_t, a1_t, s1_t, s2_t, g_head],
        scratch=[act, act, act],
        flops=10**9,
    )
    arr2 = swap(pay2, "paths")
    pay3, head_shard = call(
        net_kernel,
        [(16, 16, 128), (32, 128)],
        [path],
        [arr2, head, sets, sign, level],
        flops=10**8,
    )
    arr3 = swap(pay3, TRADES)
    pay4, g_b_mid = call(gather_kernel, [(32, 48, 128), (1, 512)], [core], [arr3], flops=10**8)
    mine = swap(pay4, "paths")
    other = lax.ppermute(mine, "trades_1", [(0, 1), (1, 0)])
    g_in, g_b_in, g_mid, pay6 = call(
        infer_kernel,
        [(64, 512), (1, 512), (512, 512), (32, 40, 128)],
        [core],
        [mine, other, w_in, b_in_r, w_mid, b_mid_r, g_b_mid, x_infer, head_shard],
        flops=10**9,
    )
    arr6 = swap(pay6, "paths")
    g_head_all, exposure = call(finish_kernel, [act, (4, 16)], [], [arr6], flops=10**6)
    return (g_in, g_b_in.reshape(-1), g_mid, g_b_mid.reshape(-1), g_head_all, exposure)


def solution(mesh):
    torus = Mesh(mesh.devices.reshape(mesh.shape["paths"], 8, 2), ("paths", "trades_0", "trades_1"))
    return jax.shard_map(
        on_device,
        mesh=torus,
        in_specs=(
            P("paths", None),
            P("paths", TRADES),
            P("paths", None),
            P(None, "paths", None),
            P(),
            P(),
            P(),
            P(),
            P(None, TRADES),
            P(TRADES),
            P(TRADES),
            P(TRADES),
        ),
        out_specs=(P(), P(), P(), P(), P(None, TRADES), P(None, TRADES)),
        check_vma=False,
    )
```

```python
import functools

import jax
import jax.numpy as jnp
from jax import lax
from jax.experimental import pallas as pl
from jax.experimental.pallas import tpu as pltpu
from jax.sharding import Mesh
from jax.sharding import PartitionSpec as P

TRADES = ("trades_0", "trades_1")
F32 = jnp.float32
BF16 = jnp.bfloat16

NN = (((1,), (0,)), ((), ()))
NT = (((1,), (1,)), ((), ()))

VALUE_SCALE = 2.0 / (8192 * 4096)
SLOPE_SCALE = 2.0 / (8192 * 64)
PORT_SCALE = 1.0 / 64.0
LEARN = 0.5

LANE_BMID = 96
LANE_BIN = 104
LANE_PORT = 105
LANE_NET = 112
LANE_NET_UPPER = 96
LANE_BIN_LATE = 64


def halves(a):
    high = a.astype(BF16)
    low = (a - high.astype(F32)).astype(BF16)
    return high, low


def mm(left, right, dims=NN):
    def dot(a, b):
        return lax.dot_general(a, b, dims, preferred_element_type=F32)

    return dot(left[0], right[0]) + (dot(left[0], right[1]) + dot(left[1], right[0]))


def softplus_sigmoid(z):
    e = jnp.exp(-jnp.abs(z))
    act = jnp.maximum(z, 0.0) + jnp.log1p(e)
    slope = jnp.where(z >= 0, 1.0, e) / (1.0 + e)
    return act, slope


def softplus(z):
    return jnp.maximum(z, 0.0) + jnp.log1p(jnp.exp(-jnp.abs(z)))


def trade_weights(sign, level):
    return (2 * sign - 1).astype(F32) * (0.5 + 0.25 * level.astype(F32))


def column_of(row):
    return jnp.broadcast_to(row, (128, row.shape[1])).T[:, 0:1]


def lane_index(shape):
    return lax.broadcasted_iota(jnp.int32, shape, len(shape) - 1)


def forward_kernel(
    path, trade, core, x_t, w_in, b_in, w_mid, b_mid, head, label, sign, level,
    pay, a1_t, s1_t, s2_t, a2_t, dv_t, w_in_t, w_mid_t,
):
    wt = w_in[...].T
    w_in_t[...] = wt
    z1 = mm(halves(wt), halves(x_t[...])) + column_of(b_in[...])
    a1, s1 = softplus_sigmoid(z1)
    a1_t[...] = a1
    s1_t[...] = s1
    mt = w_mid[...].T
    w_mid_t[...] = mt
    z2 = mm(halves(mt), halves(a1)) + column_of(b_mid[...])
    a2, s2 = softplus_sigmoid(z2)
    a2_t[...] = a2
    s2_t[...] = s2
    hd = head[...]
    hp = halves(hd)
    values = mm(halves(hd.T), halves(a2))
    err = (values - label[...].T) * VALUE_SCALE
    dv_t[...] = err
    d_a2 = mm(hp, halves(err))
    pay[:, 0:32, :] = d_a2[:, 0:128].reshape(16, 32, 128)
    pay[:, 32:64, :] = d_a2[:, 128:256].reshape(16, 32, 128)
    w = trade_weights(sign[...], level[...])
    port = jnp.sum(hd * w, axis=1, keepdims=True)
    for k in range(4):
        col = jnp.broadcast_to(port[128 * k : 128 * k + 128], (128, 128))
        row = col.T[0:1]
        pay[:, 64 + k : 65 + k, :] = jnp.broadcast_to(row[None], (16, 1, 128))
    pay[:, 68:72, :] = jnp.zeros((16, 4, 128), F32)


def head_grad_kernel(a2_t, dv_t, out):
    out[...] = mm(halves(a2_t[...]), halves(dv_t[...]), NT)


def backward_kernel(
    own, arrived, x_t, slope_label_t, w_in, w_in_t, w_mid, w_mid_t, a1_t, s1_t, s2_t, g_head,
    pay, u2_s, q_s, z_s,
):
    rows = pl.ds(pl.multiple_of(own[0] * 32, 32), 32)
    total = jnp.sum(arrived[...], axis=0)
    d_a2 = jnp.concatenate([total[0:32], total[32:64]], axis=1)
    port = jnp.concatenate(
        [column_of(total[64 + k : 65 + k]) for k in range(4)], axis=0
    ) * PORT_SCALE
    s1 = s1_t[...]
    s2 = s2_t[...]
    u2 = port * s2
    u2_s[...] = u2
    v1 = mm(halves(w_mid[...]), halves(u2))
    u1 = v1 * s1
    slopes = mm(halves(w_in[...]), halves(u1))
    d_slope = (slopes - slope_label_t[...]) * SLOPE_SCALE
    du1 = mm(halves(w_in_t[...]), halves(d_slope))
    dv1 = du1 * s1
    ds1 = du1 * v1
    dv1_p = halves(dv1)
    du2 = mm(halves(w_mid_t[...]), dv1_p)
    du2_s2 = du2 * s2
    g_port = jnp.sum(du2_s2, axis=1, keepdims=True)
    q_s[...] = du2_s2 * port * (1.0 - s2)
    dz2 = d_a2 * s2_t[rows, :] + q_s[rows, :]
    z_s[...] = jnp.zeros_like(z_s)
    z_s[rows, :] = dz2
    da1 = mm(halves(w_mid[...]), halves(z_s[...]))
    dz1 = da1 * s1 + (ds1 * s1 * (1.0 - s1)) * (1.0 / 16.0)
    g_b_in = jnp.sum(dz1, axis=1, keepdims=True)
    none = jnp.zeros((64, 256), F32)
    few = jnp.zeros((32, 256), F32)
    mid_a = jnp.concatenate([none, dz2, few], axis=0)
    mid_b = jnp.concatenate([none, u2_s[rows, :], few], axis=0)
    slope_rows = jnp.concatenate([d_slope * (1.0 / 16.0), none], axis=0)
    x_rows = jnp.concatenate([x_t[...], none], axis=0)
    ext = mm(halves(a1_t[...]), halves(mid_a), NT)
    ext = ext + mm(dv1_p, halves(mid_b), NT)
    ext = ext + mm(halves(u1), halves(slope_rows), NT)
    ext = ext + mm(halves(dz1), halves(x_rows), NT)
    lane = lane_index((512, 128))
    ext = jnp.where(lane == LANE_BIN, g_b_in, ext)
    ext = jnp.where(lane == LANE_PORT, g_port, ext)
    b_mid = jnp.sum(dz2, axis=1, keepdims=True)
    unit = lax.broadcasted_iota(jnp.int32, (32, 128), 0)
    spot = lane_index((32, 128)) == LANE_BMID + (unit & 7)
    spread = jnp.where(spot, b_mid, 0.0)
    lines = [jnp.sum(spread[8 * k : 8 * k + 8], axis=0, keepdims=True) for k in range(4)]
    tile = jnp.concatenate(lines + [jnp.zeros((4, 128), F32)], axis=0)
    blocks = ext.reshape(64, 8, 128) + tile[None]
    pay[:, 0:8, :] = blocks[0:32]
    pay[:, 8:16, :] = blocks[32:64]
    pay[:, 16:24, :] = g_head[0:256, 0:128].reshape(32, 8, 128)
    pay[:, 24:32, :] = g_head[0:256, 128:256].reshape(32, 8, 128)
    pay[:, 32:40, :] = g_head[256:512, 0:128].reshape(32, 8, 128)
    pay[:, 40:48, :] = g_head[256:512, 128:256].reshape(32, 8, 128)


def net_kernel(own, arrived, head, sets, sign, level, pay, head_shard):
    total = jnp.sum(arrived[...], axis=0)
    trunk = total[0:16]
    w = trade_weights(sign[...], level[...])
    upper = jnp.concatenate([total[16:24], total[24:32]], axis=1)
    lower = jnp.concatenate([total[32:40], total[40:48]], axis=1)
    g_head = jnp.concatenate([upper, lower], axis=0)
    g_head = g_head + trunk[:, LANE_PORT : LANE_PORT + 1] * (w * PORT_SCALE)
    head_shard[0:8, :] = g_head[0:8, 0:128]
    head_shard[8:16, :] = g_head[0:8, 128:256]
    head_shard[16:24, :] = g_head[8:16, 0:128]
    head_shard[24:32, :] = g_head[8:16, 128:256]
    first = pl.multiple_of(own[0] * 8, 8)
    second = pl.multiple_of(own[0] * 8 + 256, 8)
    old = jnp.concatenate([head[pl.ds(first, 8), :], head[pl.ds(second, 8), :]], axis=0)
    weighted = halves((old - LEARN * g_head) * w)
    ids = jnp.broadcast_to(sets[...], (128, 256))
    place = lax.broadcasted_iota(jnp.int32, (128, 256), 0) - LANE_NET
    lane = lane_index((16, 128))
    for t in range(16):
        member = ((ids == place + 16 * t) & (place >= 0)).astype(F32).astype(BF16)
        net = lax.dot_general(weighted[0], member, NT, preferred_element_type=F32)
        net = net + lax.dot_general(weighted[1], member, NT, preferred_element_type=F32)
        pay[t] = jnp.where(lane < LANE_NET, trunk, net)


def gather_kernel(own, arrived, pay, g_b_mid):
    total = jnp.sum(arrived[...], axis=0)
    lane = lane_index((16, 128))
    row_lane = lane_index((1, 128))
    first = own[0] == 0
    tiles = []
    for k in range(4):
        block = jnp.zeros((16, 128), F32)
        bias = jnp.zeros((1, 128), F32)
        for m in range(4):
            part = arrived[4 * k + m]
            moved = part if m == 2 else pltpu.roll(part, (32 * m - 64) % 128, 1)
            block = jnp.where((lane >= 32 * m) & (lane < 32 * m + 32), moved, block)
            for r in range(4):
                to = 32 * m + 8 * r
                shift = (to - LANE_BMID) % 128
                line = part[0:8] if shift == 0 else pltpu.roll(part[0:8], shift, 1)
                bias = jnp.where((row_lane >= to) & (row_lane < to + 8), line[r : r + 1], bias)
        g_b_mid[:, 128 * k : 128 * k + 128] = bias
        tiles.append(jnp.where(first, block[0:8], block[8:16]))
    upper, lower = total[0:8], total[8:16]
    own_rows = jnp.where(first, upper, lower)
    net_shift = (LANE_NET_UPPER - LANE_NET) % 128
    eight = lane_index((8, 128))
    bias_rows = pltpu.roll(own_rows, (LANE_BIN_LATE - LANE_BIN) % 128, 1)
    own_rows = jnp.where(eight < LANE_BIN_LATE, own_rows, bias_rows)
    mixed = jnp.where(eight < LANE_NET_UPPER, own_rows, pltpu.roll(upper, net_shift, 1))
    mixed = jnp.where(eight < LANE_NET, mixed, lower)
    packed = jnp.concatenate(tiles + [mixed], axis=0)
    pay[...] = jnp.broadcast_to(packed[None], (32, 40, 128))


def infer_kernel(
    own, mine, other, w_in, b_in, w_mid, b_mid, g_b_mid, x_t, head_shard,
    g_in_out, g_b_in_out, g_mid_out, pay,
):
    first = own[0] == 0
    for k in range(4):
        a = mine[:, 8 * k : 8 * k + 8, :].reshape(256, 128)
        b = other[:, 8 * k : 8 * k + 8, :].reshape(256, 128)
        g_mid_out[0:256, 128 * k : 128 * k + 128] = jnp.where(first, a, b)
        g_mid_out[256:512, 128 * k : 128 * k + 128] = jnp.where(first, b, a)
    near = mine[:, 32:40, :].reshape(256, 128)
    away = other[:, 32:40, :].reshape(256, 128)
    upper = jnp.where(first, near, away)
    lower = jnp.where(first, away, near)
    flat = jnp.concatenate([upper, lower], axis=0).T
    g_in = flat[0:64]
    g_b_in = flat[LANE_BIN_LATE : LANE_BIN_LATE + 1]
    net_shift = (LANE_NET - LANE_NET_UPPER) % 128
    both = jnp.concatenate([pltpu.roll(near, net_shift, 1), near], axis=0)
    g_in_out[...] = g_in
    g_b_in_out[...] = g_b_in
    new_in = halves(w_in[...] - LEARN * g_in)
    new_b_in = b_in[...] - LEARN * g_b_in
    new_mid = halves(w_mid[...] - LEARN * g_mid_out[...])
    new_b_mid = b_mid[...] - LEARN * g_b_mid[...]
    net_head = halves(both)
    sums = []
    for d in range(4):
        a1 = softplus(mm(halves(x_t[d].T), new_in) + new_b_in)
        a2 = softplus(mm(halves(a1), new_mid) + new_b_mid)
        netted = mm(halves(a2), net_head)
        sums.append(jnp.sum(jnp.maximum(netted, 0.0), axis=0, keepdims=True))
    tile = jnp.concatenate(sums + [jnp.zeros((4, 128), F32)], axis=0)
    pay[:, 0:32, :] = jnp.broadcast_to(head_shard[...][None], (32, 32, 128))
    pay[:, 32:40, :] = jnp.broadcast_to(tile[None], (32, 8, 128))


def finish_kernel(arrived, g_head, exposure):
    g_head[0:256, 0:128] = arrived[:, 0:8, :].reshape(256, 128)
    g_head[0:256, 128:256] = arrived[:, 8:16, :].reshape(256, 128)
    g_head[256:512, 0:128] = arrived[:, 16:24, :].reshape(256, 128)
    g_head[256:512, 128:256] = arrived[:, 24:32, :].reshape(256, 128)
    total = jnp.sum(arrived[:, 32:40, :], axis=0) * (1.0 / 8192.0)
    moved = pltpu.roll(total, 128 - LANE_NET, 1)
    exposure[...] = moved[0:4, 0:16]


def keep(a):
    return pltpu.with_memory_space_constraint(a, pltpu.VMEM)


def far(a):
    return pltpu.with_memory_space_constraint(a, pltpu.HBM)


def call(kernel, outs, scalars, args, scratch=(), flops=0, placed=(), final=(), away=()):
    shapes = tuple(
        pltpu.HBM(s, F32) if i in final else pltpu.VMEM(s, F32)
        for i, s in enumerate(outs)
    )
    vmem = pl.BlockSpec(memory_space=pltpu.VMEM)
    smem = pl.BlockSpec(memory_space=pltpu.SMEM)
    args = [keep(a) if any(a is p for p in placed) else a for a in args]
    args = [far(a) if any(a is p for p in away) else a for a in args]
    return pl.pallas_call(
        kernel,
        out_shape=shapes,
        in_specs=[smem] * len(scalars) + [vmem] * len(args),
        out_specs=tuple(vmem for _ in outs),
        scratch_shapes=[pltpu.VMEM(s, F32) for s in scratch],
        cost_estimate=pl.CostEstimate(flops=flops, transcendentals=0, bytes_accessed=0),
        compiler_params=pltpu.CompilerParams(vmem_limit_bytes=24 * 2**20),
        name=kernel.__name__,
    )(*scalars, *args)


def swap(x, axis):
    return lax.all_to_all(x, axis, 0, 0, tiled=True)


def on_device(
    x_train, value_label, slope_label, x_infer, w_in, b_in, w_mid, b_mid, head,
    trade_set, trade_sign, trade_level,
):
    path = lax.axis_index("paths").astype(jnp.int32).reshape(1)
    trade = lax.axis_index(TRADES).astype(jnp.int32).reshape(1)
    core = lax.axis_index("trades_1").astype(jnp.int32).reshape(1)
    b_in_r = b_in.reshape(1, -1)
    b_mid_r = b_mid.reshape(1, -1)
    sets = trade_set.reshape(1, -1)
    sign = trade_sign.reshape(1, -1)
    level = trade_level.reshape(1, -1)
    act = (512, 256)
    x_t = x_train.T
    slope_label_t = slope_label.T
    x_infer_t = x_infer.transpose(0, 2, 1)
    pay1, a1_t, s1_t, s2_t, a2_t, dv_t, w_in_t, w_mid_t = call(
        forward_kernel,
        [(16, 72, 128), act, act, act, act, (256, 256), (512, 64), (512, 512)],
        [path, trade, core],
        [x_t, w_in, b_in_r, w_mid, b_mid_r, head, value_label, sign, level],
        flops=10**9,
        final=(0, 2, 3, 4, 5),
        away=[x_t, w_in, w_mid, head, value_label, b_in_r, b_mid_r, sign, level],
    )
    arr1 = swap(pay1, TRADES)
    (g_head,) = call(head_grad_kernel, [act], [], [a2_t, dv_t], flops=4 * 10**8, final=(0,), away=[a2_t, dv_t])
    (pay2,) = call(
        backward_kernel,
        [(32, 48, 128)],
        [trade],
        [arr1, x_t, slope_label_t, w_in, w_in_t, w_mid, w_mid_t, a1_t, s1_t, s2_t, g_head],
        scratch=[act, act, act],
        flops=10**9,
        placed=[arr1, w_in_t, w_mid_t, a1_t, w_mid],
        away=[s1_t, s2_t, g_head, x_t, slope_label_t, w_in],
    )
    arr2 = swap(pay2, "paths")
    pay3, head_shard = call(
        net_kernel,
        [(16, 16, 128), (32, 128)],
        [path],
        [arr2, head, sets, sign, level],
        flops=10**8,
        placed=[arr2],
    )
    arr3 = swap(pay3, TRADES)
    pay4, g_b_mid = call(gather_kernel, [(32, 40, 128), (1, 512)], [core], [arr3], flops=10**8, placed=[arr3], final=(1,))
    mine = swap(pay4, "paths")
    other = lax.ppermute(mine, "trades_1", [(0, 1), (1, 0)])
    g_in, g_b_in, g_mid, pay6 = call(
        infer_kernel,
        [(64, 512), (1, 512), (512, 512), (32, 40, 128)],
        [core],
        [mine, other, w_in, b_in_r, w_mid, b_mid_r, g_b_mid, x_infer_t, head_shard],
        flops=10**9,
        placed=[mine, other, head_shard],
        final=(0, 1, 2),
    )
    arr6 = swap(pay6, "paths")
    g_head_all, exposure = call(finish_kernel, [act, (4, 16)], [], [arr6], flops=10**6, placed=[arr6], final=(0, 1))
    return (g_in, g_b_in.reshape(-1), g_mid, g_b_mid.reshape(-1), g_head_all, exposure)


def solution(mesh):
    torus = Mesh(mesh.devices.reshape(mesh.shape["paths"], 8, 2), ("paths", "trades_0", "trades_1"))
    return jax.shard_map(
        on_device,
        mesh=torus,
        in_specs=(
            P("paths", None),
            P("paths", TRADES),
            P("paths", None),
            P(None, "paths", None),
            P(),
            P(),
            P(),
            P(),
            P(None, TRADES),
            P(TRADES),
            P(TRADES),
            P(TRADES),
        ),
        out_specs=(P(), P(), P(), P(), P(None, TRADES), P(None, TRADES)),
        check_vma=False,
    )
```

```python
import functools

import jax
import jax.numpy as jnp
from jax import lax
from jax.experimental import pallas as pl
from jax.experimental.pallas import tpu as pltpu
from jax.sharding import Mesh
from jax.sharding import PartitionSpec as P

TRADES = ("trades_0", "trades_1")
PATHS = ("x", "z")
F32 = jnp.float32
BF16 = jnp.bfloat16

NN = (((1,), (0,)), ((), ()))
NT = (((1,), (1,)), ((), ()))

VALUE_SCALE = 2.0 / (8192 * 4096)
SLOPE_SCALE = 2.0 / (8192 * 64)
PORT_SCALE = 1.0 / 64.0
LEARN = 0.5

LANE_BMID = 96
LANE_BIN = 104
LANE_PORT = 105
LANE_NET = 112
LANE_NET_UPPER = 96
LANE_BIN_LATE = 64


def halves(a):
    high = a.astype(BF16)
    low = (a - high.astype(F32)).astype(BF16)
    return high, low


def mm(left, right, dims=NN):
    def dot(a, b):
        return lax.dot_general(a, b, dims, preferred_element_type=F32)

    return dot(left[0], right[0]) + (dot(left[0], right[1]) + dot(left[1], right[0]))


def softplus_sigmoid(z):
    e = jnp.exp(-jnp.abs(z))
    act = jnp.maximum(z, 0.0) + jnp.log1p(e)
    slope = jnp.where(z >= 0, 1.0, e) / (1.0 + e)
    return act, slope


def softplus(z):
    return jnp.maximum(z, 0.0) + jnp.log1p(jnp.exp(-jnp.abs(z)))


def trade_weights(sign, level):
    return (2 * sign - 1).astype(F32) * (0.5 + 0.25 * level.astype(F32))


def column_of(row):
    return jnp.broadcast_to(row, (128, row.shape[1])).T[:, 0:1]


def lane_index(shape):
    return lax.broadcasted_iota(jnp.int32, shape, len(shape) - 1)


def forward_kernel(
    path, trade, core, x_t, w_in, b_in, w_mid, b_mid, head, label, sign, level, sets,
    pay, a1_t, s1_t, s2_t, a2_t, dv_t, w_in_t, w_mid_t, small,
):
    wt = w_in[...].T
    w_in_t[...] = wt
    z1 = mm(halves(wt), halves(x_t[...])) + column_of(b_in[...])
    a1, s1 = softplus_sigmoid(z1)
    a1_t[...] = a1
    s1_t[...] = s1
    mt = w_mid[...].T
    w_mid_t[...] = mt
    z2 = mm(halves(mt), halves(a1)) + column_of(b_mid[...])
    a2, s2 = softplus_sigmoid(z2)
    a2_t[...] = a2
    s2_t[...] = s2
    hd = head[...]
    hp = halves(hd)
    values = mm(halves(hd.T), halves(a2))
    err = (values - label[...].T) * VALUE_SCALE
    dv_t[...] = err
    d_a2 = mm(hp, halves(err))
    pay[:, 0:32, :] = d_a2[:, 0:128].reshape(16, 32, 128)
    pay[:, 32:64, :] = d_a2[:, 128:256].reshape(16, 32, 128)
    w = trade_weights(sign[...], level[...])
    small[0:1, 0:256] = w
    small[1:2, 0:256] = sets[...].astype(F32)
    small[2:3, :] = b_in[...]
    small[3:4, :] = b_mid[...]
    port = jnp.sum(hd * w, axis=1, keepdims=True)
    for k in range(4):
        col = jnp.broadcast_to(port[128 * k : 128 * k + 128], (128, 128))
        row = col.T[0:1]
        pay[:, 64 + k : 65 + k, :] = jnp.broadcast_to(row[None], (16, 1, 128))
    pay[:, 68:72, :] = jnp.zeros((16, 4, 128), F32)


def head_grad_kernel(a2_t, dv_t, out):
    out[...] = mm(halves(a2_t[...]), halves(dv_t[...]), NT)


def backward_kernel(
    own, arrived, x_t, slope_label_t, w_in, w_in_t, w_mid, w_mid_t, a1_t, s1_t, s2_t, g_head,
    pay, u2_s, q_s, z_s,
):
    rows = pl.ds(pl.multiple_of(own[0] * 32, 32), 32)
    total = jnp.sum(arrived[...], axis=0)
    d_a2 = jnp.concatenate([total[0:32], total[32:64]], axis=1)
    port = jnp.concatenate(
        [column_of(total[64 + k : 65 + k]) for k in range(4)], axis=0
    ) * PORT_SCALE
    s1 = s1_t[...]
    s2 = s2_t[...]
    u2 = port * s2
    u2_s[...] = u2
    v1 = mm(halves(w_mid[...]), halves(u2))
    u1 = v1 * s1
    slopes = mm(halves(w_in[...]), halves(u1))
    d_slope = (slopes - slope_label_t[...]) * SLOPE_SCALE
    du1 = mm(halves(w_in_t[...]), halves(d_slope))
    dv1 = du1 * s1
    ds1 = du1 * v1
    dv1_p = halves(dv1)
    du2 = mm(halves(w_mid_t[...]), dv1_p)
    du2_s2 = du2 * s2
    g_port = jnp.sum(du2_s2, axis=1, keepdims=True)
    q_s[...] = du2_s2 * port * (1.0 - s2)
    dz2 = d_a2 * s2_t[rows, :] + q_s[rows, :]
    z_s[...] = jnp.zeros_like(z_s)
    z_s[rows, :] = dz2
    da1 = mm(halves(w_mid[...]), halves(z_s[...]))
    dz1 = da1 * s1 + (ds1 * s1 * (1.0 - s1)) * (1.0 / 16.0)
    g_b_in = jnp.sum(dz1, axis=1, keepdims=True)
    none = jnp.zeros((64, 256), F32)
    few = jnp.zeros((32, 256), F32)
    mid_a = jnp.concatenate([none, dz2, few], axis=0)
    mid_b = jnp.concatenate([none, u2_s[rows, :], few], axis=0)
    slope_rows = jnp.concatenate([d_slope * (1.0 / 16.0), none], axis=0)
    x_rows = jnp.concatenate([x_t[...], none], axis=0)
    ext = mm(halves(a1_t[...]), halves(mid_a), NT)
    ext = ext + mm(dv1_p, halves(mid_b), NT)
    ext = ext + mm(halves(u1), halves(slope_rows), NT)
    ext = ext + mm(halves(dz1), halves(x_rows), NT)
    lane = lane_index((512, 128))
    ext = jnp.where(lane == LANE_BIN, g_b_in, ext)
    ext = jnp.where(lane == LANE_PORT, g_port, ext)
    b_mid = jnp.sum(dz2, axis=1, keepdims=True)
    unit = lax.broadcasted_iota(jnp.int32, (32, 128), 0)
    spot = lane_index((32, 128)) == LANE_BMID + (unit & 7)
    spread = jnp.where(spot, b_mid, 0.0)
    lines = [jnp.sum(spread[8 * k : 8 * k + 8], axis=0, keepdims=True) for k in range(4)]
    tile = jnp.concatenate(lines + [jnp.zeros((4, 128), F32)], axis=0)
    blocks = ext.reshape(64, 8, 128) + tile[None]
    pay[:, 0:8, :] = blocks[0:32]
    pay[:, 8:16, :] = blocks[32:64]
    pay[:, 16:24, :] = g_head[0:256, 0:128].reshape(32, 8, 128)
    pay[:, 24:32, :] = g_head[0:256, 128:256].reshape(32, 8, 128)
    pay[:, 32:40, :] = g_head[256:512, 0:128].reshape(32, 8, 128)
    pay[:, 40:48, :] = g_head[256:512, 128:256].reshape(32, 8, 128)


def net_kernel(own, arrived, head, small, pay, head_shard):
    total = jnp.sum(arrived[...], axis=0)
    trunk = total[0:16]
    w = small[0:1, 0:256]
    upper = jnp.concatenate([total[16:24], total[24:32]], axis=1)
    lower = jnp.concatenate([total[32:40], total[40:48]], axis=1)
    g_head = jnp.concatenate([upper, lower], axis=0)
    g_head = g_head + trunk[:, LANE_PORT : LANE_PORT + 1] * (w * PORT_SCALE)
    head_shard[0:8, :] = g_head[0:8, 0:128]
    head_shard[8:16, :] = g_head[0:8, 128:256]
    head_shard[16:24, :] = g_head[8:16, 0:128]
    head_shard[24:32, :] = g_head[8:16, 128:256]
    first = pl.multiple_of(own[0] * 8, 8)
    second = pl.multiple_of(own[0] * 8 + 256, 8)
    old = jnp.concatenate([head[pl.ds(first, 8), :], head[pl.ds(second, 8), :]], axis=0)
    weighted = halves((old - LEARN * g_head) * w)
    ids = jnp.broadcast_to(small[1:2, 0:256].astype(jnp.int32), (128, 256))
    place = lax.broadcasted_iota(jnp.int32, (128, 256), 0) - LANE_NET
    lane = lane_index((16, 128))
    for t in range(16):
        member = ((ids == place + 16 * t) & (place >= 0)).astype(F32).astype(BF16)
        net = lax.dot_general(weighted[0], member, NT, preferred_element_type=F32)
        net = net + lax.dot_general(weighted[1], member, NT, preferred_element_type=F32)
        pay[t] = jnp.where(lane < LANE_NET, trunk, net)


def gather_kernel(own, arrived, head_shard, pay, g_b_mid):
    total = jnp.sum(arrived[...], axis=0)
    lane = lane_index((16, 128))
    row_lane = lane_index((1, 128))
    first = own[0] == 0
    tiles = []
    for k in range(4):
        block = jnp.zeros((16, 128), F32)
        bias = jnp.zeros((1, 128), F32)
        for m in range(4):
            part = arrived[4 * k + m]
            moved = part if m == 2 else pltpu.roll(part, (32 * m - 64) % 128, 1)
            block = jnp.where((lane >= 32 * m) & (lane < 32 * m + 32), moved, block)
            for r in range(4):
                to = 32 * m + 8 * r
                shift = (to - LANE_BMID) % 128
                line = part[0:8] if shift == 0 else pltpu.roll(part[0:8], shift, 1)
                bias = jnp.where((row_lane >= to) & (row_lane < to + 8), line[r : r + 1], bias)
        g_b_mid[:, 128 * k : 128 * k + 128] = bias
        tiles.append(jnp.where(first, block[0:8], block[8:16]))
    upper, lower = total[0:8], total[8:16]
    own_rows = jnp.where(first, upper, lower)
    net_shift = (LANE_NET_UPPER - LANE_NET) % 128
    eight = lane_index((8, 128))
    bias_rows = pltpu.roll(own_rows, (LANE_BIN_LATE - LANE_BIN) % 128, 1)
    own_rows = jnp.where(eight < LANE_BIN_LATE, own_rows, bias_rows)
    mixed = jnp.where(eight < LANE_NET_UPPER, own_rows, pltpu.roll(upper, net_shift, 1))
    mixed = jnp.where(eight < LANE_NET, mixed, lower)
    packed = jnp.concatenate(tiles + [mixed, head_shard[...]], axis=0)
    pay[...] = jnp.broadcast_to(packed[None], (8, 72, 128))


def spread_kernel(arrived, trunk, head):
    lines = arrived[:, 0:40, :].reshape(320, 128)
    trunk[...] = jnp.broadcast_to(lines[None], (4, 320, 128))
    heads = arrived[:, 40:72, :].reshape(256, 128)
    head[...] = jnp.broadcast_to(heads[None], (4, 256, 128))


def infer_kernel(
    own, mine, other, w_in, w_mid, small, g_b_mid, x_t,
    g_in_out, g_b_in_out, g_mid_out, pay,
):
    first = own[0] == 0
    for k in range(4):
        a = mine[:, 8 * k : 8 * k + 8, :].reshape(256, 128)
        b = other[:, 8 * k : 8 * k + 8, :].reshape(256, 128)
        g_mid_out[0:256, 128 * k : 128 * k + 128] = jnp.where(first, a, b)
        g_mid_out[256:512, 128 * k : 128 * k + 128] = jnp.where(first, b, a)
    near = mine[:, 32:40, :].reshape(256, 128)
    away = other[:, 32:40, :].reshape(256, 128)
    upper = jnp.where(first, near, away)
    lower = jnp.where(first, away, near)
    flat = jnp.concatenate([upper, lower], axis=0).T
    g_in = flat[0:64]
    g_b_in = flat[LANE_BIN_LATE : LANE_BIN_LATE + 1]
    net_shift = (LANE_NET - LANE_NET_UPPER) % 128
    both = jnp.concatenate([pltpu.roll(near, net_shift, 1), near], axis=0)
    g_in_out[...] = g_in
    g_b_in_out[...] = g_b_in
    new_in = halves(w_in[...] - LEARN * g_in)
    new_b_in = small[2:3, :] - LEARN * g_b_in
    new_mid = halves(w_mid[...] - LEARN * g_mid_out[...])
    new_b_mid = small[3:4, :] - LEARN * g_b_mid[...]
    net_head = halves(both)
    row = jnp.zeros((1, 128), F32)
    lane = lane_index((1, 128))
    for d in range(4):
        a1 = softplus(mm(halves(x_t[d].T), new_in) + new_b_in)
        a2 = softplus(mm(halves(a1), new_mid) + new_b_mid)
        netted = mm(halves(a2), net_head)
        line = jnp.sum(jnp.maximum(netted, 0.0), axis=0, keepdims=True)
        moved = pltpu.roll(line, (16 * d - LANE_NET) % 128, 1)
        row = jnp.where((lane >= 16 * d) & (lane < 16 * d + 16), moved, row)
    pay[...] = jnp.broadcast_to(row[None], (32, 1, 128))


def finish_kernel(arrived, lines, g_head, exposure):
    g_head[0:256, 0:128] = arrived[:, 0:8, :].reshape(256, 128)
    g_head[0:256, 128:256] = arrived[:, 8:16, :].reshape(256, 128)
    g_head[256:512, 0:128] = arrived[:, 16:24, :].reshape(256, 128)
    g_head[256:512, 128:256] = arrived[:, 24:32, :].reshape(256, 128)
    total = jnp.sum(lines[...], axis=0) * (1.0 / 8192.0)
    for d in range(4):
        moved = total if d == 0 else pltpu.roll(total, 128 - 16 * d, 1)
        exposure[d : d + 1, :] = moved[:, 0:16]


def keep(a):
    return pltpu.with_memory_space_constraint(a, pltpu.VMEM)


def far(a):
    return pltpu.with_memory_space_constraint(a, pltpu.HBM)


def call(kernel, outs, scalars, args, scratch=(), flops=0, placed=(), final=(), away=()):
    shapes = tuple(
        pltpu.HBM(s, F32) if i in final else pltpu.VMEM(s, F32)
        for i, s in enumerate(outs)
    )
    vmem = pl.BlockSpec(memory_space=pltpu.VMEM)
    smem = pl.BlockSpec(memory_space=pltpu.SMEM)
    args = [keep(a) if any(a is p for p in placed) else a for a in args]
    args = [far(a) if any(a is p for p in away) else a for a in args]
    return pl.pallas_call(
        kernel,
        out_shape=shapes,
        in_specs=[smem] * len(scalars) + [vmem] * len(args),
        out_specs=tuple(vmem for _ in outs),
        scratch_shapes=[pltpu.VMEM(s, F32) for s in scratch],
        cost_estimate=pl.CostEstimate(flops=flops, transcendentals=0, bytes_accessed=0),
        compiler_params=pltpu.CompilerParams(vmem_limit_bytes=24 * 2**20),
        name=kernel.__name__,
    )(*scalars, *args)


def swap(x, axis):
    return lax.all_to_all(x, axis, 0, 0, tiled=True)


def on_device(
    x_train, value_label, slope_label, x_infer, w_in, b_in, w_mid, b_mid, head,
    trade_set, trade_sign, trade_level,
):
    path = lax.axis_index(PATHS).astype(jnp.int32).reshape(1)
    trade = lax.axis_index(TRADES).astype(jnp.int32).reshape(1)
    core = lax.axis_index("trades_1").astype(jnp.int32).reshape(1)
    b_in_r = b_in.reshape(1, -1)
    b_mid_r = b_mid.reshape(1, -1)
    sets = trade_set.reshape(1, -1)
    sign = trade_sign.reshape(1, -1)
    level = trade_level.reshape(1, -1)
    act = (512, 256)
    x_t = x_train.T
    slope_label_t = slope_label.T
    x_infer_t = x_infer.transpose(0, 2, 1)
    pay1, a1_t, s1_t, s2_t, a2_t, dv_t, w_in_t, w_mid_t, small = call(
        forward_kernel,
        [(16, 72, 128), act, act, act, act, (256, 256), (512, 64), (512, 512), (8, 512)],
        [path, trade, core],
        [x_t, w_in, b_in_r, w_mid, b_mid_r, head, value_label, sign, level, sets],
        flops=10**9,
        final=(0, 2, 3, 4, 5),
        away=[x_t, w_in, w_mid, head, value_label, b_in_r, b_mid_r, sign, level, sets],
    )
    arr1 = swap(pay1, TRADES)
    (g_head,) = call(head_grad_kernel, [act], [], [a2_t, dv_t], flops=4 * 10**8, final=(0,), away=[a2_t, dv_t])
    (pay2,) = call(
        backward_kernel,
        [(32, 48, 128)],
        [trade],
        [arr1, x_t, slope_label_t, w_in, w_in_t, w_mid, w_mid_t, a1_t, s1_t, s2_t, g_head],
        scratch=[act, act, act],
        flops=10**9,
        placed=[arr1, w_in_t, w_mid_t, a1_t, w_mid],
        away=[s1_t, s2_t, g_head, x_t, slope_label_t, w_in],
    )
    arr2 = swap(pay2, PATHS)
    pay3, head_shard = call(
        net_kernel,
        [(16, 16, 128), (32, 128)],
        [path],
        [arr2, head, small],
        flops=10**8,
        placed=[arr2, small],
    )
    arr3 = swap(pay3, TRADES)
    pay4, g_b_mid = call(
        gather_kernel,
        [(8, 72, 128), (1, 512)],
        [core],
        [arr3, head_shard],
        flops=10**8,
        placed=[arr3, head_shard],
        final=(1,),
    )
    arr4 = swap(pay4, "z")
    pay5, pay_head = call(
        spread_kernel, [(4, 320, 128), (4, 256, 128)], [], [arr4], flops=10**6, placed=[arr4]
    )
    mine = swap(pay5, "x").reshape(32, 40, 128)
    pay_head, mine = lax.optimization_barrier((pay_head, mine))
    arr_head = swap(pay_head, "x").reshape(32, 32, 128)
    other = lax.ppermute(mine, "trades_1", [(0, 1), (1, 0)])
    g_in, g_b_in, g_mid, pay6 = call(
        infer_kernel,
        [(64, 512), (1, 512), (512, 512), (32, 1, 128)],
        [core],
        [mine, other, w_in, w_mid, small, g_b_mid, x_infer_t],
        flops=10**9,
        placed=[mine, other, small],
        final=(0, 1, 2),
    )
    arr6 = swap(pay6, PATHS)
    g_head_all, exposure = call(
        finish_kernel,
        [act, (4, 16)],
        [],
        [arr_head, arr6],
        flops=10**6,
        placed=[arr_head, arr6],
        final=(0, 1),
    )
    return (g_in, g_b_in.reshape(-1), g_mid, g_b_mid.reshape(-1), g_head_all, exposure)


def solution(mesh):
    torus = Mesh(mesh.devices.reshape(4, 8, 8, 2), PATHS + TRADES)
    return jax.shard_map(
        on_device,
        mesh=torus,
        in_specs=(
            P(PATHS, None),
            P(PATHS, TRADES),
            P(PATHS, None),
            P(None, PATHS, None),
            P(),
            P(),
            P(),
            P(),
            P(None, TRADES),
            P(TRADES),
            P(TRADES),
            P(TRADES),
        ),
        out_specs=(P(), P(), P(), P(), P(None, TRADES), P(None, TRADES)),
        check_vma=False,
    )
```

```python
import functools

import jax
import jax.numpy as jnp
from jax import lax
from jax.experimental import pallas as pl
from jax.experimental.pallas import tpu as pltpu
from jax.sharding import Mesh
from jax.sharding import PartitionSpec as P

TRADES = ("trades_0", "trades_1")
PATHS = ("x", "z")
F32 = jnp.float32
BF16 = jnp.bfloat16

NN = (((1,), (0,)), ((), ()))
NT = (((1,), (1,)), ((), ()))

VALUE_SCALE = 2.0 / (8192 * 4096)
SLOPE_SCALE = 2.0 / (8192 * 64)
PORT_SCALE = 1.0 / 64.0
LEARN = 0.5

LANE_BMID = 96
LANE_BIN = 104
LANE_PORT = 105
LANE_NET = 112
LANE_NET_UPPER = 96
LANE_BIN_LATE = 64


def halves(a):
    high = a.astype(BF16)
    low = (a - high.astype(F32)).astype(BF16)
    return high, low


def mm(left, right, dims=NN):
    def dot(a, b):
        return lax.dot_general(a, b, dims, preferred_element_type=F32)

    return dot(left[0], right[0]) + (dot(left[0], right[1]) + dot(left[1], right[0]))


def softplus(z):
    return jnp.maximum(z, 0.0) + jnp.log(1.0 + jnp.exp(-jnp.abs(z)))


def trade_weights(sign, level):
    return (2 * sign - 1).astype(F32) * (0.5 + 0.25 * level.astype(F32))


def column_of(row):
    return jnp.broadcast_to(row, (128, row.shape[1])).T[:, 0:1]


def lane_index(shape):
    return lax.broadcasted_iota(jnp.int32, shape, len(shape) - 1)


def forward_kernel(
    path, trade, core, x_t, w_in, b_in, w_mid, b_mid, head, label, sign, level, sets,
    own, other, a1_t, a2_t, dv_t, w_mid_t, small,
):
    first = core[0] == 0
    wt = w_in[...].T
    z1 = mm(halves(wt), halves(x_t[...])) + column_of(b_in[...])
    a1 = softplus(z1)
    a1_t[...] = a1
    mt = w_mid[...].T
    w_mid_t[...] = mt
    z2 = mm(halves(mt), halves(a1)) + column_of(b_mid[...])
    a2 = softplus(z2)
    a2_t[...] = a2
    hd = head[...]
    values = mm(halves(hd.T), halves(a2))
    err = (values - label[...].T) * VALUE_SCALE
    dv_t[...] = err
    err_p = halves(err)
    d_a2 = mm(halves(hd), err_p)
    w = trade_weights(sign[...], level[...])

    def place(block, rows, start):
        pairs = block.reshape(8, 2, rows, 128)
        even = pairs[:, 0]
        odd = pairs[:, 1]
        own[:, start : start + rows, :] = jnp.where(first, even, odd)
        other[:, start : start + rows, :] = jnp.where(first, odd, even)

    place(d_a2[:, 0:128], 32, 0)
    place(d_a2[:, 128:256], 32, 32)
    small[0:1, 0:256] = w
    small[1:2, 0:256] = sets[...].astype(F32)
    small[2:3, :] = b_in[...]
    small[3:4, :] = b_mid[...]
    port = jnp.sum(hd * w, axis=1, keepdims=True)
    rows = []
    for k in range(4):
        col = jnp.broadcast_to(port[128 * k : 128 * k + 128], (128, 128))
        rows.append(col.T[0:1])
    tile = jnp.concatenate(rows + [jnp.zeros((4, 128), F32)], axis=0)
    own[:, 64:72, :] = jnp.broadcast_to(tile[None], (8, 8, 128))
    other[:, 64:72, :] = jnp.broadcast_to(tile[None], (8, 8, 128))


def join_kernel(own, got, out):
    out[...] = own[...] + got[...]


def head_grad_kernel(a2_t, dv_t, out):
    out[...] = mm(halves(a2_t[...]), halves(dv_t[...]), NT)


def backward_kernel(
    own, arrived, x_t, slope_label_t, w_in, w_mid, w_mid_t, a1_t, a2_t, g_head,
    pay, s2_s, u2_s, q_s, z_s,
):
    rows = pl.ds(pl.multiple_of(own[0] * 32, 32), 32)
    total = jnp.sum(arrived[...], axis=0)
    d_a2 = jnp.concatenate([total[0:32], total[32:64]], axis=1)
    port = jnp.concatenate(
        [column_of(total[64 + k : 65 + k]) for k in range(4)], axis=0
    ) * PORT_SCALE
    a1 = a1_t[...]
    a2 = a2_t[...]
    s1 = 1.0 - jnp.exp(-a1)
    s2 = 1.0 - jnp.exp(-a2)
    s2_s[...] = s2
    u2 = port * s2
    u2_s[...] = u2
    mid_p = halves(w_mid[...])
    v1 = mm(mid_p, halves(u2))
    u1 = v1 * s1
    slopes = mm(halves(w_in[...]), halves(u1))
    d_slope = (slopes - slope_label_t[...]) * SLOPE_SCALE
    du1 = mm(halves(w_in[...].T), halves(d_slope))
    dv1 = du1 * s1
    ds1 = du1 * v1
    dv1_p = halves(dv1)
    du2 = mm(halves(w_mid_t[...]), dv1_p)
    du2_s2 = du2 * s2
    g_port = jnp.sum(du2_s2, axis=1, keepdims=True)
    q_s[...] = du2_s2 * port * (1.0 - s2)
    dz2 = d_a2 * s2_s[rows, :] + q_s[rows, :]
    z_s[...] = jnp.zeros_like(z_s)
    z_s[rows, :] = dz2
    da1 = mm(mid_p, halves(z_s[...]))
    dz1 = da1 * s1 + (ds1 * s1 * (1.0 - s1)) * (1.0 / 16.0)
    g_b_in = jnp.sum(dz1, axis=1, keepdims=True)
    none = jnp.zeros((64, 256), F32)
    few = jnp.zeros((32, 256), F32)
    mid_a = jnp.concatenate([none, dz2, few], axis=0)
    mid_b = jnp.concatenate([none, u2_s[rows, :], few], axis=0)
    slope_rows = jnp.concatenate([d_slope * (1.0 / 16.0), none], axis=0)
    x_rows = jnp.concatenate([x_t[...], none], axis=0)
    ext = mm(halves(a1), halves(mid_a), NT)
    ext = ext + mm(dv1_p, halves(mid_b), NT)
    ext = ext + mm(halves(u1), halves(slope_rows), NT)
    ext = ext + mm(halves(dz1), halves(x_rows), NT)
    lane = lane_index((512, 128))
    ext = jnp.where(lane == LANE_BIN, g_b_in, ext)
    ext = jnp.where(lane == LANE_PORT, g_port, ext)
    b_mid = jnp.sum(dz2, axis=1, keepdims=True)
    unit = lax.broadcasted_iota(jnp.int32, (32, 128), 0)
    spot = lane_index((32, 128)) == LANE_BMID + (unit & 7)
    spread = jnp.where(spot, b_mid, 0.0)
    lines = [jnp.sum(spread[8 * k : 8 * k + 8], axis=0, keepdims=True) for k in range(4)]
    tile = jnp.concatenate(lines + [jnp.zeros((4, 128), F32)], axis=0)
    blocks = ext.reshape(64, 8, 128) + tile[None]
    pay[:, 0:8, :] = blocks[0:32]
    pay[:, 8:16, :] = blocks[32:64]
    pay[:, 16:24, :] = g_head[0:256, 0:128].reshape(32, 8, 128)
    pay[:, 24:32, :] = g_head[0:256, 128:256].reshape(32, 8, 128)
    pay[:, 32:40, :] = g_head[256:512, 0:128].reshape(32, 8, 128)
    pay[:, 40:48, :] = g_head[256:512, 128:256].reshape(32, 8, 128)


def net_kernel(own, arrived, head, small, pay, head_shard):
    total = jnp.sum(arrived[...], axis=0)
    trunk = total[0:16]
    w = small[0:1, 0:256]
    upper = jnp.concatenate([total[16:24], total[24:32]], axis=1)
    lower = jnp.concatenate([total[32:40], total[40:48]], axis=1)
    g_head = jnp.concatenate([upper, lower], axis=0)
    g_head = g_head + trunk[:, LANE_PORT : LANE_PORT + 1] * (w * PORT_SCALE)
    head_shard[0:8, :] = g_head[0:8, 0:128]
    head_shard[8:16, :] = g_head[0:8, 128:256]
    head_shard[16:24, :] = g_head[8:16, 0:128]
    head_shard[24:32, :] = g_head[8:16, 128:256]
    first = pl.multiple_of(own[0] * 8, 8)
    second = pl.multiple_of(own[0] * 8 + 256, 8)
    old = jnp.concatenate([head[pl.ds(first, 8), :], head[pl.ds(second, 8), :]], axis=0)
    weighted = halves((old - LEARN * g_head) * w)
    ids = jnp.broadcast_to(small[1:2, 0:256].astype(jnp.int32), (128, 256))
    place = lax.broadcasted_iota(jnp.int32, (128, 256), 0) - LANE_NET
    lane = lane_index((16, 128))
    for t in range(16):
        member = ((ids == place + 16 * t) & (place >= 0)).astype(F32).astype(BF16)
        net = lax.dot_general(weighted[0], member, NT, preferred_element_type=F32)
        net = net + lax.dot_general(weighted[1], member, NT, preferred_element_type=F32)
        pay[t] = jnp.where(lane < LANE_NET, trunk, net)


def gather_kernel(own, arrived, head_shard, pay, g_b_mid):
    total = jnp.sum(arrived[...], axis=0)
    lane = lane_index((16, 128))
    row_lane = lane_index((1, 128))
    first = own[0] == 0
    tiles = []
    for k in range(4):
        block = jnp.zeros((16, 128), F32)
        bias = jnp.zeros((1, 128), F32)
        for m in range(4):
            part = arrived[4 * k + m]
            moved = part if m == 2 else pltpu.roll(part, (32 * m - 64) % 128, 1)
            block = jnp.where((lane >= 32 * m) & (lane < 32 * m + 32), moved, block)
            for r in range(4):
                to = 32 * m + 8 * r
                shift = (to - LANE_BMID) % 128
                line = part[0:8] if shift == 0 else pltpu.roll(part[0:8], shift, 1)
                bias = jnp.where((row_lane >= to) & (row_lane < to + 8), line[r : r + 1], bias)
        g_b_mid[:, 128 * k : 128 * k + 128] = bias
        tiles.append(jnp.where(first, block[0:8], block[8:16]))
    upper, lower = total[0:8], total[8:16]
    own_rows = jnp.where(first, upper, lower)
    net_shift = (LANE_NET_UPPER - LANE_NET) % 128
    eight = lane_index((8, 128))
    bias_rows = pltpu.roll(own_rows, (LANE_BIN_LATE - LANE_BIN) % 128, 1)
    own_rows = jnp.where(eight < LANE_BIN_LATE, own_rows, bias_rows)
    mixed = jnp.where(eight < LANE_NET_UPPER, own_rows, pltpu.roll(upper, net_shift, 1))
    mixed = jnp.where(eight < LANE_NET, mixed, lower)
    packed = jnp.concatenate(tiles + [mixed, head_shard[...]], axis=0)
    pay[...] = jnp.broadcast_to(packed[None], (8, 72, 128))


def spread_kernel(arrived, trunk, head):
    lines = arrived[:, 0:40, :].reshape(320, 128)
    trunk[...] = jnp.broadcast_to(lines[None], (4, 320, 128))
    heads = arrived[:, 40:72, :].reshape(256, 128)
    head[...] = jnp.broadcast_to(heads[None], (4, 256, 128))


def infer_kernel(
    own, mine, other, w_in, w_mid, small, g_b_mid, x_t,
    g_in_out, g_b_in_out, g_mid_out, pay,
):
    first = own[0] == 0
    for k in range(4):
        a = mine[:, 8 * k : 8 * k + 8, :].reshape(256, 128)
        b = other[:, 8 * k : 8 * k + 8, :].reshape(256, 128)
        g_mid_out[0:256, 128 * k : 128 * k + 128] = jnp.where(first, a, b)
        g_mid_out[256:512, 128 * k : 128 * k + 128] = jnp.where(first, b, a)
    near = mine[:, 32:40, :].reshape(256, 128)
    away = other[:, 32:40, :].reshape(256, 128)
    upper = jnp.where(first, near, away)
    lower = jnp.where(first, away, near)
    flat = jnp.concatenate([upper, lower], axis=0).T
    g_in = flat[0:64]
    g_b_in = flat[LANE_BIN_LATE : LANE_BIN_LATE + 1]
    net_shift = (LANE_NET - LANE_NET_UPPER) % 128
    both = jnp.concatenate([pltpu.roll(near, net_shift, 1), near], axis=0)
    g_in_out[...] = g_in
    g_b_in_out[...] = g_b_in
    new_in = halves(w_in[...] - LEARN * g_in)
    deep_in = jnp.concatenate([new_in[0], new_in[0], new_in[1]], axis=0)
    new_b_in = small[2:3, :] - LEARN * g_b_in
    new_mid = halves(w_mid[...] - LEARN * g_mid_out[...])
    new_b_mid = small[3:4, :] - LEARN * g_b_mid[...]
    net_head = halves(both)
    row = jnp.zeros((1, 128), F32)
    lane = lane_index((1, 128))
    for d in range(4):
        high, low = halves(x_t[d].T)
        rows = jnp.concatenate([high, low, high], axis=1)
        first_pre = jnp.dot(rows, deep_in, preferred_element_type=F32)
        a1 = softplus(first_pre + new_b_in)
        a2 = softplus(mm(halves(a1), new_mid) + new_b_mid)
        netted = mm(halves(a2), net_head)
        line = jnp.sum(jnp.maximum(netted, 0.0), axis=0, keepdims=True)
        moved = pltpu.roll(line, (16 * d - LANE_NET) % 128, 1)
        row = jnp.where((lane >= 16 * d) & (lane < 16 * d + 16), moved, row)
    pay[...] = jnp.broadcast_to(row[None], (32, 1, 128))


def finish_kernel(arrived, lines, g_head, exposure):
    g_head[0:256, 0:128] = arrived[:, 0:8, :].reshape(256, 128)
    g_head[0:256, 128:256] = arrived[:, 8:16, :].reshape(256, 128)
    g_head[256:512, 0:128] = arrived[:, 16:24, :].reshape(256, 128)
    g_head[256:512, 128:256] = arrived[:, 24:32, :].reshape(256, 128)
    total = jnp.sum(lines[...], axis=0) * (1.0 / 8192.0)
    for d in range(4):
        moved = total if d == 0 else pltpu.roll(total, 128 - 16 * d, 1)
        exposure[d : d + 1, :] = moved[:, 0:16]


def keep(a):
    return pltpu.with_memory_space_constraint(a, pltpu.VMEM)


def far(a):
    return pltpu.with_memory_space_constraint(a, pltpu.HBM)


def call(kernel, outs, scalars, args, scratch=(), flops=0, placed=(), final=(), away=()):
    shapes = tuple(
        pltpu.HBM(s, F32) if i in final else pltpu.VMEM(s, F32)
        for i, s in enumerate(outs)
    )
    vmem = pl.BlockSpec(memory_space=pltpu.VMEM)
    smem = pl.BlockSpec(memory_space=pltpu.SMEM)
    args = [keep(a) if any(a is p for p in placed) else a for a in args]
    args = [far(a) if any(a is p for p in away) else a for a in args]
    return pl.pallas_call(
        kernel,
        out_shape=shapes,
        in_specs=[smem] * len(scalars) + [vmem] * len(args),
        out_specs=tuple(vmem for _ in outs),
        scratch_shapes=[pltpu.VMEM(s, F32) for s in scratch],
        cost_estimate=pl.CostEstimate(flops=flops, transcendentals=0, bytes_accessed=0),
        compiler_params=pltpu.CompilerParams(vmem_limit_bytes=24 * 2**20),
        name=kernel.__name__,
    )(*scalars, *args)


def swap(x, axis):
    return lax.all_to_all(x, axis, 0, 0, tiled=True)


def on_device(
    x_train, value_label, slope_label, x_infer, w_in, b_in, w_mid, b_mid, head,
    trade_set, trade_sign, trade_level,
):
    path = lax.axis_index(PATHS).astype(jnp.int32).reshape(1)
    trade = lax.axis_index(TRADES).astype(jnp.int32).reshape(1)
    core = lax.axis_index("trades_1").astype(jnp.int32).reshape(1)
    b_in_r = b_in.reshape(1, -1)
    b_mid_r = b_mid.reshape(1, -1)
    sets = trade_set.reshape(1, -1)
    sign = trade_sign.reshape(1, -1)
    level = trade_level.reshape(1, -1)
    act = (512, 256)
    x_t = x_train.T
    slope_label_t = slope_label.T
    x_infer_t = x_infer.transpose(0, 2, 1)
    own, other, a1_t, a2_t, dv_t, w_mid_t, small = call(
        forward_kernel,
        [(8, 72, 128), (8, 72, 128), act, act, (256, 256), (512, 512), (8, 512)],
        [path, trade, core],
        [x_t, w_in, b_in_r, w_mid, b_mid_r, head, value_label, sign, level, sets],
        flops=10**9,
        final=(4,),
        away=[x_t, w_in, w_mid, head, value_label, b_in_r, b_mid_r, sign, level, sets],
    )
    got = lax.ppermute(other, "trades_1", [(0, 1), (1, 0)])
    (g_head,) = call(
        head_grad_kernel,
        [act],
        [],
        [a2_t, dv_t],
        flops=4 * 10**8,
        placed=[a2_t],
        away=[dv_t],
        final=(0,),
    )
    (pay1,) = call(join_kernel, [(8, 72, 128)], [], [own, got], flops=10**6, placed=[own, got])
    pay1, g_head = lax.optimization_barrier((pay1, g_head))
    arr1 = swap(pay1, "trades_0")
    (pay2,) = call(
        backward_kernel,
        [(32, 48, 128)],
        [trade],
        [arr1, x_t, slope_label_t, w_in, w_mid, w_mid_t, a1_t, a2_t, g_head],
        scratch=[act, act, act, act],
        flops=10**9,
        placed=[arr1, w_mid_t, a1_t, a2_t],
        away=[x_t, slope_label_t, w_in, g_head],
    )
    arr2 = swap(pay2, PATHS)
    pay3, head_shard = call(
        net_kernel,
        [(16, 16, 128), (32, 128)],
        [path],
        [arr2, head, small],
        flops=10**8,
        placed=[arr2, small],
    )
    arr3 = swap(pay3, TRADES)
    pay4, g_b_mid = call(
        gather_kernel,
        [(8, 72, 128), (1, 512)],
        [core],
        [arr3, head_shard],
        flops=10**8,
        placed=[arr3, head_shard],
        final=(1,),
    )
    arr4 = swap(pay4, "z")
    pay5, pay_head = call(
        spread_kernel, [(4, 320, 128), (4, 256, 128)], [], [arr4], flops=10**6, placed=[arr4]
    )
    mine = swap(pay5, "x").reshape(32, 40, 128)
    pay_head, mine = lax.optimization_barrier((pay_head, mine))
    arr_head = swap(pay_head, "x").reshape(32, 32, 128)
    other = lax.ppermute(mine, "trades_1", [(0, 1), (1, 0)])
    g_in, g_b_in, g_mid, pay6 = call(
        infer_kernel,
        [(64, 512), (1, 512), (512, 512), (32, 1, 128)],
        [core],
        [mine, other, w_in, w_mid, small, g_b_mid, x_infer_t],
        flops=10**9,
        placed=[mine, other, small],
        final=(0, 1, 2),
    )
    arr6 = swap(pay6, PATHS)
    g_head_all, exposure = call(
        finish_kernel,
        [act, (4, 16)],
        [],
        [arr_head, arr6],
        flops=10**6,
        placed=[arr_head, arr6],
        final=(0, 1),
    )
    return (g_in, g_b_in.reshape(-1), g_mid, g_b_mid.reshape(-1), g_head_all, exposure)


def solution(mesh):
    torus = Mesh(mesh.devices.reshape(4, 8, 8, 2), PATHS + TRADES)
    return jax.shard_map(
        on_device,
        mesh=torus,
        in_specs=(
            P(PATHS, None),
            P(PATHS, TRADES),
            P(PATHS, None),
            P(None, PATHS, None),
            P(),
            P(),
            P(),
            P(),
            P(None, TRADES),
            P(TRADES),
            P(TRADES),
            P(TRADES),
        ),
        out_specs=(P(), P(), P(), P(), P(None, TRADES), P(None, TRADES)),
        check_vma=False,
    )
```

```python
import functools

import jax
import jax.numpy as jnp
from jax import lax
from jax.experimental import pallas as pl
from jax.experimental.pallas import tpu as pltpu
from jax.sharding import Mesh
from jax.sharding import PartitionSpec as P

TRADES = ("trades_0", "trades_1")
PATHS = ("x", "z")
F32 = jnp.float32
BF16 = jnp.bfloat16

NN = (((1,), (0,)), ((), ()))
NT = (((1,), (1,)), ((), ()))

VALUE_SCALE = 2.0 / (8192 * 4096)
SLOPE_SCALE = 2.0 / (8192 * 64)
PORT_SCALE = 1.0 / 64.0
LEARN = 0.5

LANE_BMID = 96
LANE_BIN = 104
LANE_PORT = 105
LANE_NET = 112
LANE_NET_UPPER = 96
LANE_BIN_LATE = 64


def halves(a):
    high = a.astype(BF16)
    low = (a - high.astype(F32)).astype(BF16)
    return high, low


def mm(left, right, dims=NN):
    def dot(a, b):
        return lax.dot_general(a, b, dims, preferred_element_type=F32)

    return dot(left[0], right[0]) + (dot(left[0], right[1]) + dot(left[1], right[0]))


def mm_narrow(left, right, dims=NN):
    both = jnp.concatenate(right, axis=1 if dims is NN else 0)
    wide = lax.dot_general(left[0], both, dims, preferred_element_type=F32)
    rest = lax.dot_general(left[1], right[0], dims, preferred_element_type=F32)
    return wide[:, 0:128] + (wide[:, 128:256] + rest)


def softplus(z):
    return jnp.maximum(z, 0.0) + jnp.log(1.0 + jnp.exp(-jnp.abs(z)))


def trade_weights(sign, level):
    return (2 * sign - 1).astype(F32) * (0.5 + 0.25 * level.astype(F32))


def column_of(row):
    return jnp.broadcast_to(row, (128, row.shape[1])).T[:, 0:1]


def lane_index(shape):
    return lax.broadcasted_iota(jnp.int32, shape, len(shape) - 1)


def forward_kernel(
    path, trade, core, x_t, w_in, b_in, w_mid, b_mid, head, label, sign, level, sets,
    own, other, a1_t, a2_t, dv_t, small,
):
    first = core[0] == 0
    wt = w_in[...].T
    z1 = mm(halves(wt), halves(x_t[...])) + column_of(b_in[...])
    a1 = softplus(z1)
    a1_t[...] = a1
    mt = w_mid[...].T
    z2 = mm(halves(mt), halves(a1)) + column_of(b_mid[...])
    a2 = softplus(z2)
    a2_t[...] = a2
    hd = head[...]
    values = mm(halves(hd.T), halves(a2))
    err = (values - label[...].T) * VALUE_SCALE
    dv_t[...] = err
    err_p = halves(err)
    d_a2 = mm(halves(hd), err_p)
    w = trade_weights(sign[...], level[...])

    def place(block, rows, start):
        pairs = block.reshape(8, 2, rows, 128)
        even = pairs[:, 0]
        odd = pairs[:, 1]
        own[:, start : start + rows, :] = jnp.where(first, even, odd)
        other[:, start : start + rows, :] = jnp.where(first, odd, even)

    place(d_a2[:, 0:128], 32, 0)
    place(d_a2[:, 128:256], 32, 32)
    small[0:1, 0:256] = w
    small[1:2, 0:256] = sets[...].astype(F32)
    small[2:3, :] = b_in[...]
    small[3:4, :] = b_mid[...]
    port = jnp.sum(hd * w, axis=1, keepdims=True)
    rows = []
    for k in range(4):
        col = jnp.broadcast_to(port[128 * k : 128 * k + 128], (128, 128))
        rows.append(col.T[0:1])
    tile = jnp.concatenate(rows + [jnp.zeros((4, 128), F32)], axis=0)
    own[:, 64:72, :] = jnp.broadcast_to(tile[None], (8, 8, 128))
    other[:, 64:72, :] = jnp.broadcast_to(tile[None], (8, 8, 128))


def join_kernel(own, got, out):
    out[...] = own[...] + got[...]


def head_grad_kernel(a2_t, dv_t, out):
    out[...] = mm(halves(a2_t[...]), halves(dv_t[...]), NT)


def backward_kernel(
    own, arrived, x_t, slope_label_t, w_in, w_mid, a1_t, a2_t, g_head,
    pay, s2_s, u2_s, q_s, z_s,
):
    rows = pl.ds(pl.multiple_of(own[0] * 32, 32), 32)
    total = jnp.sum(arrived[...], axis=0)
    d_a2 = jnp.concatenate([total[0:32], total[32:64]], axis=1)
    port = jnp.concatenate(
        [column_of(total[64 + k : 65 + k]) for k in range(4)], axis=0
    ) * PORT_SCALE
    a1 = a1_t[...]
    a2 = a2_t[...]
    s1 = 1.0 - jnp.exp(-a1)
    s2 = 1.0 - jnp.exp(-a2)
    s2_s[...] = s2
    u2 = port * s2
    u2_s[...] = u2
    mid_p = halves(w_mid[...])
    v1 = mm(mid_p, halves(u2))
    u1 = v1 * s1
    slopes = mm(halves(w_in[...]), halves(u1))
    d_slope = (slopes - slope_label_t[...]) * SLOPE_SCALE
    du1 = mm(halves(w_in[...].T), halves(d_slope))
    dv1 = du1 * s1
    ds1 = du1 * v1
    dv1_p = halves(dv1)
    du2 = mm(halves(w_mid[...].T), dv1_p)
    du2_s2 = du2 * s2
    g_port = jnp.sum(du2_s2, axis=1, keepdims=True)
    q_s[...] = du2_s2 * port * (1.0 - s2)
    dz2 = d_a2 * s2_s[rows, :] + q_s[rows, :]
    z_s[...] = jnp.zeros_like(z_s)
    z_s[rows, :] = dz2
    da1 = mm(mid_p, halves(z_s[...]))
    dz1 = da1 * s1 + (ds1 * s1 * (1.0 - s1)) * (1.0 / 16.0)
    g_b_in = jnp.sum(dz1, axis=1, keepdims=True)
    none = jnp.zeros((64, 256), F32)
    few = jnp.zeros((32, 256), F32)
    mid_a = jnp.concatenate([none, dz2, few], axis=0)
    mid_b = jnp.concatenate([none, u2_s[rows, :], few], axis=0)
    slope_rows = jnp.concatenate([d_slope * (1.0 / 16.0), none], axis=0)
    x_rows = jnp.concatenate([x_t[...], none], axis=0)
    ext = mm_narrow(halves(a1), halves(mid_a), NT)
    ext = ext + mm_narrow(dv1_p, halves(mid_b), NT)
    ext = ext + mm_narrow(halves(u1), halves(slope_rows), NT)
    ext = ext + mm_narrow(halves(dz1), halves(x_rows), NT)
    lane = lane_index((512, 128))
    ext = jnp.where(lane == LANE_BIN, g_b_in, ext)
    ext = jnp.where(lane == LANE_PORT, g_port, ext)
    b_mid = jnp.sum(dz2, axis=1, keepdims=True)
    unit = lax.broadcasted_iota(jnp.int32, (32, 128), 0)
    spot = lane_index((32, 128)) == LANE_BMID + (unit & 7)
    spread = jnp.where(spot, b_mid, 0.0)
    lines = [jnp.sum(spread[8 * k : 8 * k + 8], axis=0, keepdims=True) for k in range(4)]
    tile = jnp.concatenate(lines + [jnp.zeros((4, 128), F32)], axis=0)
    blocks = ext.reshape(64, 8, 128) + tile[None]
    pay[:, 0:8, :] = blocks[0:32]
    pay[:, 8:16, :] = blocks[32:64]
    pay[:, 16:24, :] = g_head[0:256, 0:128].reshape(32, 8, 128)
    pay[:, 24:32, :] = g_head[0:256, 128:256].reshape(32, 8, 128)
    pay[:, 32:40, :] = g_head[256:512, 0:128].reshape(32, 8, 128)
    pay[:, 40:48, :] = g_head[256:512, 128:256].reshape(32, 8, 128)


def net_kernel(own, arrived, head, small, pay, head_shard):
    total = jnp.sum(arrived[...], axis=0)
    trunk = total[0:16]
    w = small[0:1, 0:256]
    upper = jnp.concatenate([total[16:24], total[24:32]], axis=1)
    lower = jnp.concatenate([total[32:40], total[40:48]], axis=1)
    g_head = jnp.concatenate([upper, lower], axis=0)
    g_head = g_head + trunk[:, LANE_PORT : LANE_PORT + 1] * (w * PORT_SCALE)
    head_shard[0:8, :] = g_head[0:8, 0:128]
    head_shard[8:16, :] = g_head[0:8, 128:256]
    head_shard[16:24, :] = g_head[8:16, 0:128]
    head_shard[24:32, :] = g_head[8:16, 128:256]
    first = pl.multiple_of(own[0] * 8, 8)
    second = pl.multiple_of(own[0] * 8 + 256, 8)
    old = jnp.concatenate([head[pl.ds(first, 8), :], head[pl.ds(second, 8), :]], axis=0)
    weighted = halves((old - LEARN * g_head) * w)
    ids = jnp.broadcast_to(small[1:2, 0:256].astype(jnp.int32), (128, 256))
    place = lax.broadcasted_iota(jnp.int32, (128, 256), 0) - LANE_NET
    lane = lane_index((16, 128))
    for t in range(16):
        member = ((ids == place + 16 * t) & (place >= 0)).astype(F32).astype(BF16)
        net = lax.dot_general(weighted[0], member, NT, preferred_element_type=F32)
        net = net + lax.dot_general(weighted[1], member, NT, preferred_element_type=F32)
        pay[t] = jnp.where(lane < LANE_NET, trunk, net)


def gather_kernel(own, arrived, head_shard, pay, g_b_mid, g_b_near):
    total = jnp.sum(arrived[...], axis=0)
    lane = lane_index((16, 128))
    row_lane = lane_index((1, 128))
    first = own[0] == 0
    tiles = []
    for k in range(4):
        block = jnp.zeros((16, 128), F32)
        bias = jnp.zeros((1, 128), F32)
        for m in range(4):
            part = arrived[4 * k + m]
            moved = part if m == 2 else pltpu.roll(part, (32 * m - 64) % 128, 1)
            block = jnp.where((lane >= 32 * m) & (lane < 32 * m + 32), moved, block)
            for r in range(4):
                to = 32 * m + 8 * r
                shift = (to - LANE_BMID) % 128
                line = part[0:8] if shift == 0 else pltpu.roll(part[0:8], shift, 1)
                bias = jnp.where((row_lane >= to) & (row_lane < to + 8), line[r : r + 1], bias)
        g_b_mid[:, 128 * k : 128 * k + 128] = bias
        g_b_near[:, 128 * k : 128 * k + 128] = bias
        tiles.append(jnp.where(first, block[0:8], block[8:16]))
    upper, lower = total[0:8], total[8:16]
    own_rows = jnp.where(first, upper, lower)
    net_shift = (LANE_NET_UPPER - LANE_NET) % 128
    eight = lane_index((8, 128))
    bias_rows = pltpu.roll(own_rows, (LANE_BIN_LATE - LANE_BIN) % 128, 1)
    own_rows = jnp.where(eight < LANE_BIN_LATE, own_rows, bias_rows)
    mixed = jnp.where(eight < LANE_NET_UPPER, own_rows, pltpu.roll(upper, net_shift, 1))
    mixed = jnp.where(eight < LANE_NET, mixed, lower)
    packed = jnp.concatenate(tiles + [mixed, head_shard[...]], axis=0)
    pay[...] = jnp.broadcast_to(packed[None], (8, 72, 128))


def spread_kernel(arrived, out):
    lines = arrived[...].reshape(576, 128)
    out[...] = jnp.broadcast_to(lines[None], (4, 576, 128))


def head_out_kernel(arrived, g_head):
    g_head[0:256, 0:128] = arrived[:, 40:48, :].reshape(256, 128)
    g_head[0:256, 128:256] = arrived[:, 48:56, :].reshape(256, 128)
    g_head[256:512, 0:128] = arrived[:, 56:64, :].reshape(256, 128)
    g_head[256:512, 128:256] = arrived[:, 64:72, :].reshape(256, 128)


def infer_kernel(
    own, mine, other, w_in, w_mid, small, g_b_mid, x_t,
    g_in_out, g_b_in_out, g_mid_out, pay,
):
    first = own[0] == 0
    for k in range(4):
        a = mine[:, 8 * k : 8 * k + 8, :].reshape(256, 128)
        b = other[:, 8 * k : 8 * k + 8, :].reshape(256, 128)
        g_mid_out[0:256, 128 * k : 128 * k + 128] = jnp.where(first, a, b)
        g_mid_out[256:512, 128 * k : 128 * k + 128] = jnp.where(first, b, a)
    near = mine[:, 32:40, :].reshape(256, 128)
    away = other[:, 32:40, :].reshape(256, 128)
    upper = jnp.where(first, near, away)
    lower = jnp.where(first, away, near)
    flat = jnp.concatenate([upper, lower], axis=0).T
    g_in = flat[0:64]
    g_b_in = flat[LANE_BIN_LATE : LANE_BIN_LATE + 1]
    net_shift = (LANE_NET - LANE_NET_UPPER) % 128
    both = jnp.concatenate([pltpu.roll(near, net_shift, 1), near], axis=0)
    g_in_out[...] = g_in
    g_b_in_out[...] = g_b_in
    new_in = halves(w_in[...] - LEARN * g_in)
    deep_in = jnp.concatenate([new_in[0], new_in[0], new_in[1]], axis=0)
    new_b_in = small[2:3, :] - LEARN * g_b_in
    new_mid = halves(w_mid[...] - LEARN * g_mid_out[...])
    new_b_mid = small[3:4, :] - LEARN * g_b_mid[...]
    net_head = halves(both)
    row = jnp.zeros((1, 128), F32)
    lane = lane_index((1, 128))
    for d in range(4):
        high, low = halves(x_t[d].T)
        rows = jnp.concatenate([high, low, high], axis=1)
        first_pre = jnp.dot(rows, deep_in, preferred_element_type=F32)
        a1 = softplus(first_pre + new_b_in)
        a2 = softplus(mm(halves(a1), new_mid) + new_b_mid)
        netted = mm_narrow(halves(a2), net_head)
        line = jnp.sum(jnp.maximum(netted, 0.0), axis=0, keepdims=True)
        moved = pltpu.roll(line, (16 * d - LANE_NET) % 128, 1)
        row = jnp.where((lane >= 16 * d) & (lane < 16 * d + 16), moved, row)
    pay[...] = jnp.broadcast_to(row[None], (32, 1, 128))


def finish_kernel(lines, exposure):
    total = jnp.sum(lines[...], axis=0) * (1.0 / 8192.0)
    for d in range(4):
        moved = total if d == 0 else pltpu.roll(total, 128 - 16 * d, 1)
        exposure[d : d + 1, :] = moved[:, 0:16]


def keep(a):
    return pltpu.with_memory_space_constraint(a, pltpu.VMEM)


def far(a):
    return pltpu.with_memory_space_constraint(a, pltpu.HBM)


def call(kernel, outs, scalars, args, scratch=(), flops=0, placed=(), final=(), away=()):
    shapes = tuple(
        pltpu.HBM(s, F32) if i in final else pltpu.VMEM(s, F32)
        for i, s in enumerate(outs)
    )
    vmem = pl.BlockSpec(memory_space=pltpu.VMEM)
    smem = pl.BlockSpec(memory_space=pltpu.SMEM)
    args = [keep(a) if any(a is p for p in placed) else a for a in args]
    args = [far(a) if any(a is p for p in away) else a for a in args]
    return pl.pallas_call(
        kernel,
        out_shape=shapes,
        in_specs=[smem] * len(scalars) + [vmem] * len(args),
        out_specs=tuple(vmem for _ in outs),
        scratch_shapes=[pltpu.VMEM(s, F32) for s in scratch],
        cost_estimate=pl.CostEstimate(flops=flops, transcendentals=0, bytes_accessed=0),
        compiler_params=pltpu.CompilerParams(vmem_limit_bytes=24 * 2**20),
        name=kernel.__name__,
    )(*scalars, *args)


def swap(x, axis):
    return lax.all_to_all(x, axis, 0, 0, tiled=True)


def on_device(
    x_train, value_label, slope_label, x_infer, w_in, b_in, w_mid, b_mid, head,
    trade_set, trade_sign, trade_level,
):
    path = lax.axis_index(PATHS).astype(jnp.int32).reshape(1)
    trade = lax.axis_index(TRADES).astype(jnp.int32).reshape(1)
    core = lax.axis_index("trades_1").astype(jnp.int32).reshape(1)
    b_in_r = b_in.reshape(1, -1)
    b_mid_r = b_mid.reshape(1, -1)
    sets = trade_set.reshape(1, -1)
    sign = trade_sign.reshape(1, -1)
    level = trade_level.reshape(1, -1)
    act = (512, 256)
    x_t = x_train.T
    slope_label_t = slope_label.T
    x_infer_t = x_infer.transpose(0, 2, 1)
    own, other, a1_t, a2_t, dv_t, small = call(
        forward_kernel,
        [(8, 72, 128), (8, 72, 128), act, act, (256, 256), (8, 512)],
        [path, trade, core],
        [x_t, w_in, b_in_r, w_mid, b_mid_r, head, value_label, sign, level, sets],
        flops=10**9,
        away=[x_t, w_in, w_mid, head, value_label, b_in_r, b_mid_r, sign, level, sets],
    )
    got = lax.ppermute(other, "trades_1", [(0, 1), (1, 0)])
    (g_head,) = call(
        head_grad_kernel,
        [act],
        [],
        [a2_t, dv_t],
        flops=4 * 10**8,
        placed=[a2_t, dv_t],
    )
    (pay1,) = call(join_kernel, [(8, 72, 128)], [], [own, got], flops=10**6, placed=[own, got])
    pay1, g_head = lax.optimization_barrier((pay1, g_head))
    arr1 = swap(pay1, "trades_0")
    (pay2,) = call(
        backward_kernel,
        [(32, 48, 128)],
        [trade],
        [arr1, x_t, slope_label_t, w_in, w_mid, a1_t, a2_t, g_head],
        scratch=[act, act, act, act],
        flops=10**9,
        placed=[arr1, w_mid, a1_t, a2_t, g_head, x_t, slope_label_t, w_in],
    )
    arr2 = swap(pay2, PATHS)
    pay3, head_shard = call(
        net_kernel,
        [(16, 16, 128), (32, 128)],
        [path],
        [arr2, head, small],
        flops=10**8,
        placed=[arr2, small],
    )
    arr3 = swap(pay3, TRADES)
    pay4, g_b_mid, g_b_near = call(
        gather_kernel,
        [(8, 72, 128), (1, 512), (1, 512)],
        [core],
        [arr3, head_shard],
        flops=10**8,
        placed=[arr3, head_shard],
        final=(1,),
    )
    arr4 = swap(pay4, "z")
    (pay5,) = call(spread_kernel, [(4, 576, 128)], [], [arr4], flops=10**6, placed=[arr4])
    mine = swap(pay5, "x").reshape(32, 72, 128)
    other = lax.ppermute(mine, "trades_1", [(0, 1), (1, 0)])
    (g_head_all,) = call(
        head_out_kernel, [act], [], [mine], flops=10**8, placed=[mine], final=(0,)
    )
    other, g_head_all = lax.optimization_barrier((other, g_head_all))
    g_in, g_b_in, g_mid, pay6 = call(
        infer_kernel,
        [(64, 512), (1, 512), (512, 512), (32, 1, 128)],
        [core],
        [mine, other, w_in, w_mid, small, g_b_near, x_infer_t],
        flops=10**9,
        placed=[mine, other, small, g_b_near],
        final=(0, 1, 2),
    )
    arr6 = swap(pay6, PATHS)
    (exposure,) = call(
        finish_kernel, [(4, 16)], [], [arr6], flops=10**6, placed=[arr6], final=(0,)
    )
    return (g_in, g_b_in.reshape(-1), g_mid, g_b_mid.reshape(-1), g_head_all, exposure)


def solution(mesh):
    torus = Mesh(mesh.devices.reshape(4, 8, 8, 2), PATHS + TRADES)
    return jax.shard_map(
        on_device,
        mesh=torus,
        in_specs=(
            P(PATHS, None),
            P(PATHS, TRADES),
            P(PATHS, None),
            P(None, PATHS, None),
            P(),
            P(),
            P(),
            P(),
            P(None, TRADES),
            P(TRADES),
            P(TRADES),
            P(TRADES),
        ),
        out_specs=(P(), P(), P(), P(), P(None, TRADES), P(None, TRADES)),
        check_vma=False,
    )
```

```python
import functools

import jax
import jax.numpy as jnp
from jax import lax
from jax.experimental import pallas as pl
from jax.experimental.pallas import tpu as pltpu
from jax.sharding import Mesh
from jax.sharding import PartitionSpec as P

TRADES = ("trades_0", "trades_1")
PATHS = ("x", "z")
F32 = jnp.float32
BF16 = jnp.bfloat16

NN = (((1,), (0,)), ((), ()))
NT = (((1,), (1,)), ((), ()))

VALUE_SCALE = 2.0 / (8192 * 4096)
SLOPE_SCALE = 2.0 / (8192 * 64)
PORT_SCALE = 1.0 / 64.0
LEARN = 0.5

LANE_BMID = 96
LANE_BIN = 104
LANE_PORT = 105
LANE_NET = 112
LANE_NET_UPPER = 96
LANE_BIN_LATE = 64


def halves(a):
    high = a.astype(BF16)
    low = (a - high.astype(F32)).astype(BF16)
    return high, low


def mm(left, right, dims=NN):
    def dot(a, b):
        return lax.dot_general(a, b, dims, preferred_element_type=F32)

    return dot(left[0], right[0]) + (dot(left[0], right[1]) + dot(left[1], right[0]))


def mm_narrow(left, right, dims=NN):
    both = jnp.concatenate(right, axis=1 if dims is NN else 0)
    wide = lax.dot_general(left[0], both, dims, preferred_element_type=F32)
    rest = lax.dot_general(left[1], right[0], dims, preferred_element_type=F32)
    return wide[:, 0:128] + (wide[:, 128:256] + rest)


def softplus(z):
    return jnp.maximum(z, 0.0) + jnp.log(1.0 + jnp.exp(-jnp.abs(z)))


def trade_weights(sign, level):
    return (2 * sign - 1).astype(F32) * (0.5 + 0.25 * level.astype(F32))


def column_of(row):
    return jnp.broadcast_to(row, (128, row.shape[1])).T[:, 0:1]


def lane_index(shape):
    return lax.broadcasted_iota(jnp.int32, shape, len(shape) - 1)


def forward_kernel(
    path, trade, core, x_t, w_in, b_in, w_mid, b_mid, head, label, sign, level, sets,
    own, other, a1_t, a2_t, dv_t, small,
):
    first = core[0] == 0
    wt = w_in[...].T
    z1 = mm(halves(wt), halves(x_t[...])) + column_of(b_in[...])
    a1 = softplus(z1)
    a1_t[...] = a1
    mt = w_mid[...].T
    z2 = mm(halves(mt), halves(a1)) + column_of(b_mid[...])
    a2 = softplus(z2)
    a2_t[...] = a2
    hd = head[...]
    values = mm(halves(hd.T), halves(a2))
    err = (values - label[...].T) * VALUE_SCALE
    dv_t[...] = err
    err_p = halves(err)
    d_a2 = mm(halves(hd), err_p)
    w = trade_weights(sign[...], level[...])

    def place(block, rows, start):
        pairs = block.reshape(8, 2, rows, 128)
        even = pairs[:, 0]
        odd = pairs[:, 1]
        own[:, start : start + rows, :] = jnp.where(first, even, odd)
        other[:, start : start + rows, :] = jnp.where(first, odd, even)

    place(d_a2[:, 0:128], 32, 0)
    place(d_a2[:, 128:256], 32, 32)
    small[0:1, 0:256] = w
    small[1:2, 0:256] = sets[...].astype(F32)
    small[2:3, :] = b_in[...]
    small[3:4, :] = b_mid[...]
    port = jnp.sum(hd * w, axis=1, keepdims=True)
    rows = []
    for k in range(4):
        col = jnp.broadcast_to(port[128 * k : 128 * k + 128], (128, 128))
        rows.append(col.T[0:1])
    tile = jnp.concatenate(rows + [jnp.zeros((4, 128), F32)], axis=0)
    own[:, 64:72, :] = jnp.broadcast_to(tile[None], (8, 8, 128))
    other[:, 64:72, :] = jnp.broadcast_to(tile[None], (8, 8, 128))


def join_kernel(own, got, out):
    out[...] = own[...] + got[...]


def head_grad_kernel(a2_t, dv_t, out):
    out[...] = mm(halves(a2_t[...]), halves(dv_t[...]), NT)


def backward_kernel(
    own, arrived, x_t, slope_label_t, w_in, w_mid, a1_t, a2_t, g_head,
    pay, s2_s, u2_s, q_s, z_s,
):
    rows = pl.ds(pl.multiple_of(own[0] * 32, 32), 32)
    total = jnp.sum(arrived[...], axis=0)
    d_a2 = jnp.concatenate([total[0:32], total[32:64]], axis=1)
    port = jnp.concatenate(
        [column_of(total[64 + k : 65 + k]) for k in range(4)], axis=0
    ) * PORT_SCALE
    a1 = a1_t[...]
    a2 = a2_t[...]
    s1 = 1.0 - jnp.exp(-a1)
    s2 = 1.0 - jnp.exp(-a2)
    s2_s[...] = s2
    u2 = port * s2
    u2_s[...] = u2
    mid_p = halves(w_mid[...])
    v1 = mm(mid_p, halves(u2))
    u1 = v1 * s1
    slopes = mm(halves(w_in[...]), halves(u1))
    d_slope = (slopes - slope_label_t[...]) * SLOPE_SCALE
    du1 = mm(halves(w_in[...].T), halves(d_slope))
    dv1 = du1 * s1
    ds1 = du1 * v1
    dv1_p = halves(dv1)
    du2 = mm(halves(w_mid[...].T), dv1_p)
    du2_s2 = du2 * s2
    g_port = jnp.sum(du2_s2, axis=1, keepdims=True)
    q_s[...] = du2_s2 * port * (1.0 - s2)
    dz2 = d_a2 * s2_s[rows, :] + q_s[rows, :]
    z_s[...] = jnp.zeros_like(z_s)
    z_s[rows, :] = dz2
    da1 = mm(mid_p, halves(z_s[...]))
    dz1 = da1 * s1 + (ds1 * s1 * (1.0 - s1)) * (1.0 / 16.0)
    g_b_in = jnp.sum(dz1, axis=1, keepdims=True)
    none = jnp.zeros((64, 256), F32)
    few = jnp.zeros((32, 256), F32)
    mid_a = jnp.concatenate([none, dz2, few], axis=0)
    mid_b = jnp.concatenate([none, u2_s[rows, :], few], axis=0)
    slope_rows = jnp.concatenate([d_slope * (1.0 / 16.0), none], axis=0)
    x_rows = jnp.concatenate([x_t[...], none], axis=0)
    ext = mm_narrow(halves(a1), halves(mid_a), NT)
    ext = ext + mm_narrow(dv1_p, halves(mid_b), NT)
    ext = ext + mm_narrow(halves(u1), halves(slope_rows), NT)
    ext = ext + mm_narrow(halves(dz1), halves(x_rows), NT)
    lane = lane_index((512, 128))
    ext = jnp.where(lane == LANE_BIN, g_b_in, ext)
    ext = jnp.where(lane == LANE_PORT, g_port, ext)
    b_mid = jnp.sum(dz2, axis=1, keepdims=True)
    unit = lax.broadcasted_iota(jnp.int32, (32, 128), 0)
    spot = lane_index((32, 128)) == LANE_BMID + (unit & 7)
    spread = jnp.where(spot, b_mid, 0.0)
    lines = [jnp.sum(spread[8 * k : 8 * k + 8], axis=0, keepdims=True) for k in range(4)]
    tile = jnp.concatenate(lines + [jnp.zeros((4, 128), F32)], axis=0)
    blocks = ext.reshape(64, 8, 128) + tile[None]
    pay[:, 0:8, :] = blocks[0:32]
    pay[:, 8:16, :] = blocks[32:64]
    pay[:, 16:24, :] = g_head[0:256, 0:128].reshape(32, 8, 128)
    pay[:, 24:32, :] = g_head[0:256, 128:256].reshape(32, 8, 128)
    pay[:, 32:40, :] = g_head[256:512, 0:128].reshape(32, 8, 128)
    pay[:, 40:48, :] = g_head[256:512, 128:256].reshape(32, 8, 128)


def net_kernel(own, arrived, head, small, pay, head_shard):
    total = jnp.sum(arrived[...], axis=0)
    trunk = total[0:16]
    w = small[0:1, 0:256]
    upper = jnp.concatenate([total[16:24], total[24:32]], axis=1)
    lower = jnp.concatenate([total[32:40], total[40:48]], axis=1)
    g_head = jnp.concatenate([upper, lower], axis=0)
    g_head = g_head + trunk[:, LANE_PORT : LANE_PORT + 1] * (w * PORT_SCALE)
    head_shard[0:8, :] = g_head[0:8, 0:128]
    head_shard[8:16, :] = g_head[0:8, 128:256]
    head_shard[16:24, :] = g_head[8:16, 0:128]
    head_shard[24:32, :] = g_head[8:16, 128:256]
    first = pl.multiple_of(own[0] * 8, 8)
    second = pl.multiple_of(own[0] * 8 + 256, 8)
    old = jnp.concatenate([head[pl.ds(first, 8), :], head[pl.ds(second, 8), :]], axis=0)
    weighted = halves((old - LEARN * g_head) * w)
    ids = jnp.broadcast_to(small[1:2, 0:256].astype(jnp.int32), (128, 256))
    place = lax.broadcasted_iota(jnp.int32, (128, 256), 0) - LANE_NET
    lane = lane_index((16, 128))
    for t in range(16):
        member = ((ids == place + 16 * t) & (place >= 0)).astype(F32).astype(BF16)
        net = lax.dot_general(weighted[0], member, NT, preferred_element_type=F32)
        net = net + lax.dot_general(weighted[1], member, NT, preferred_element_type=F32)
        pay[t] = jnp.where(lane < LANE_NET, trunk, net)


def gather_kernel(own, arrived, head_shard, pay, g_b_mid, g_b_near):
    total = jnp.sum(arrived[...], axis=0)
    lane = lane_index((16, 128))
    row_lane = lane_index((1, 128))
    first = own[0] == 0
    tiles = []
    for k in range(4):
        block = jnp.zeros((16, 128), F32)
        bias = jnp.zeros((1, 128), F32)
        for m in range(4):
            part = arrived[4 * k + m]
            moved = part if m == 2 else pltpu.roll(part, (32 * m - 64) % 128, 1)
            block = jnp.where((lane >= 32 * m) & (lane < 32 * m + 32), moved, block)
            for r in range(4):
                to = 32 * m + 8 * r
                shift = (to - LANE_BMID) % 128
                line = part[0:8] if shift == 0 else pltpu.roll(part[0:8], shift, 1)
                bias = jnp.where((row_lane >= to) & (row_lane < to + 8), line[r : r + 1], bias)
        g_b_mid[:, 128 * k : 128 * k + 128] = bias
        g_b_near[:, 128 * k : 128 * k + 128] = bias
        tiles.append(jnp.where(first, block[0:8], block[8:16]))
    upper, lower = total[0:8], total[8:16]
    own_rows = jnp.where(first, upper, lower)
    net_shift = (LANE_NET_UPPER - LANE_NET) % 128
    eight = lane_index((8, 128))
    bias_rows = pltpu.roll(own_rows, (LANE_BIN_LATE - LANE_BIN) % 128, 1)
    own_rows = jnp.where(eight < LANE_BIN_LATE, own_rows, bias_rows)
    mixed = jnp.where(eight < LANE_NET_UPPER, own_rows, pltpu.roll(upper, net_shift, 1))
    mixed = jnp.where(eight < LANE_NET, mixed, lower)
    packed = jnp.concatenate(tiles + [mixed, head_shard[...]], axis=0)
    pay[...] = jnp.broadcast_to(packed[None], (8, 72, 128))


def spread_kernel(arrived, out):
    lines = arrived[...].reshape(576, 128)
    out[...] = jnp.broadcast_to(lines[None], (4, 576, 128))


def trim_kernel(arrived, out):
    out[...] = arrived[:, 0:40, :]


def head_out_kernel(arrived, g_head):
    g_head[0:256, 0:128] = arrived[:, 40:48, :].reshape(256, 128)
    g_head[0:256, 128:256] = arrived[:, 48:56, :].reshape(256, 128)
    g_head[256:512, 0:128] = arrived[:, 56:64, :].reshape(256, 128)
    g_head[256:512, 128:256] = arrived[:, 64:72, :].reshape(256, 128)


def infer_kernel(
    own, mine, other, w_in, w_mid, small, g_b_mid, x_t,
    g_in_out, g_b_in_out, g_mid_out, pay, g_in_s, g_b_in_s, g_mid_s, sems,
):
    first = own[0] == 0
    for k in range(4):
        a = mine[:, 8 * k : 8 * k + 8, :].reshape(256, 128)
        b = other[:, 8 * k : 8 * k + 8, :].reshape(256, 128)
        g_mid_s[0:256, 128 * k : 128 * k + 128] = jnp.where(first, a, b)
        g_mid_s[256:512, 128 * k : 128 * k + 128] = jnp.where(first, b, a)
    near = mine[:, 32:40, :].reshape(256, 128)
    away = other[:, 32:40, :].reshape(256, 128)
    upper = jnp.where(first, near, away)
    lower = jnp.where(first, away, near)
    flat = jnp.concatenate([upper, lower], axis=0).T
    g_in = flat[0:64]
    g_b_in = flat[LANE_BIN_LATE : LANE_BIN_LATE + 1]
    net_shift = (LANE_NET - LANE_NET_UPPER) % 128
    both = jnp.concatenate([pltpu.roll(near, net_shift, 1), near], axis=0)
    g_in_s[...] = g_in
    g_b_in_s[...] = g_b_in
    copies = [
        pltpu.make_async_copy(g_mid_s, g_mid_out, sems.at[0]),
        pltpu.make_async_copy(g_in_s, g_in_out, sems.at[1]),
        pltpu.make_async_copy(g_b_in_s, g_b_in_out, sems.at[2]),
    ]
    for copy in copies:
        copy.start()
    new_in = halves(w_in[...] - LEARN * g_in)
    deep_in = jnp.concatenate([new_in[0], new_in[0], new_in[1]], axis=0)
    new_b_in = small[2:3, :] - LEARN * g_b_in
    new_mid = halves(w_mid[...] - LEARN * g_mid_s[...])
    new_b_mid = small[3:4, :] - LEARN * g_b_mid[...]
    net_head = halves(both)
    row = jnp.zeros((1, 128), F32)
    lane = lane_index((1, 128))
    for d in range(4):
        high, low = halves(x_t[d].T)
        rows = jnp.concatenate([high, low, high], axis=1)
        first_pre = jnp.dot(rows, deep_in, preferred_element_type=F32)
        a1 = softplus(first_pre + new_b_in)
        a2 = softplus(mm(halves(a1), new_mid) + new_b_mid)
        netted = mm_narrow(halves(a2), net_head)
        line = jnp.sum(jnp.maximum(netted, 0.0), axis=0, keepdims=True)
        moved = pltpu.roll(line, (16 * d - LANE_NET) % 128, 1)
        row = jnp.where((lane >= 16 * d) & (lane < 16 * d + 16), moved, row)
    pay[...] = jnp.broadcast_to(row[None], (32, 1, 128))
    for copy in copies:
        copy.wait()


def finish_kernel(lines, exposure):
    total = jnp.sum(lines[...], axis=0) * (1.0 / 8192.0)
    for d in range(4):
        moved = total if d == 0 else pltpu.roll(total, 128 - 16 * d, 1)
        exposure[d : d + 1, :] = moved[:, 0:16]


def keep(a):
    return pltpu.with_memory_space_constraint(a, pltpu.VMEM)


def far(a):
    return pltpu.with_memory_space_constraint(a, pltpu.HBM)


def call(kernel, outs, scalars, args, scratch=(), flops=0, placed=(), final=(), away=(), copies=0):
    shapes = tuple(
        pltpu.HBM(s, F32) if i in final else pltpu.VMEM(s, F32)
        for i, s in enumerate(outs)
    )
    semaphores = [pltpu.SemaphoreType.DMA((copies,))] if copies else []
    vmem = pl.BlockSpec(memory_space=pltpu.VMEM)
    smem = pl.BlockSpec(memory_space=pltpu.SMEM)
    args = [keep(a) if any(a is p for p in placed) else a for a in args]
    args = [far(a) if any(a is p for p in away) else a for a in args]
    return pl.pallas_call(
        kernel,
        out_shape=shapes,
        in_specs=[smem] * len(scalars) + [vmem] * len(args),
        out_specs=tuple(
            pl.BlockSpec(memory_space=pl.ANY) if i < copies else vmem for i in range(len(outs))
        ),
        scratch_shapes=[pltpu.VMEM(s, F32) for s in scratch] + semaphores,
        cost_estimate=pl.CostEstimate(flops=flops, transcendentals=0, bytes_accessed=0),
        compiler_params=pltpu.CompilerParams(vmem_limit_bytes=24 * 2**20),
        name=kernel.__name__,
    )(*scalars, *args)


def swap(x, axis):
    return lax.all_to_all(x, axis, 0, 0, tiled=True)


def on_device(
    x_train, value_label, slope_label, x_infer, w_in, b_in, w_mid, b_mid, head,
    trade_set, trade_sign, trade_level,
):
    path = lax.axis_index(PATHS).astype(jnp.int32).reshape(1)
    trade = lax.axis_index(TRADES).astype(jnp.int32).reshape(1)
    core = lax.axis_index("trades_1").astype(jnp.int32).reshape(1)
    b_in_r = b_in.reshape(1, -1)
    b_mid_r = b_mid.reshape(1, -1)
    sets = trade_set.reshape(1, -1)
    sign = trade_sign.reshape(1, -1)
    level = trade_level.reshape(1, -1)
    act = (512, 256)
    x_t = x_train.T
    slope_label_t = slope_label.T
    x_infer_t = x_infer.transpose(0, 2, 1)
    own, other, a1_t, a2_t, dv_t, small = call(
        forward_kernel,
        [(8, 72, 128), (8, 72, 128), act, act, (256, 256), (8, 512)],
        [path, trade, core],
        [x_t, w_in, b_in_r, w_mid, b_mid_r, head, value_label, sign, level, sets],
        flops=10**9,
        away=[x_t, w_in, w_mid, head, value_label, b_in_r, b_mid_r, sign, level, sets],
    )
    got = lax.ppermute(other, "trades_1", [(0, 1), (1, 0)])
    (g_head,) = call(
        head_grad_kernel,
        [act],
        [],
        [a2_t, dv_t],
        flops=4 * 10**8,
        placed=[a2_t, dv_t],
    )
    (pay1,) = call(join_kernel, [(8, 72, 128)], [], [own, got], flops=10**6, placed=[own, got])
    pay1, g_head = lax.optimization_barrier((pay1, g_head))
    arr1 = swap(pay1, "trades_0")
    (pay2,) = call(
        backward_kernel,
        [(32, 48, 128)],
        [trade],
        [arr1, x_t, slope_label_t, w_in, w_mid, a1_t, a2_t, g_head],
        scratch=[act, act, act, act],
        flops=10**9,
        placed=[arr1, w_mid, a1_t, a2_t, g_head, x_t, slope_label_t, w_in],
    )
    arr2 = swap(pay2, PATHS)
    pay3, head_shard = call(
        net_kernel,
        [(16, 16, 128), (32, 128)],
        [path],
        [arr2, head, small],
        flops=10**8,
        placed=[arr2, small],
    )
    arr3 = swap(pay3, TRADES)
    pay4, g_b_mid, g_b_near = call(
        gather_kernel,
        [(8, 72, 128), (1, 512), (1, 512)],
        [core],
        [arr3, head_shard],
        flops=10**8,
        placed=[arr3, head_shard],
        final=(1,),
    )
    arr4 = swap(pay4, "z")
    (pay5,) = call(spread_kernel, [(4, 576, 128)], [], [arr4], flops=10**6, placed=[arr4])
    mine = swap(pay5, "x").reshape(32, 72, 128)
    (trunk,) = call(trim_kernel, [(32, 40, 128)], [], [mine], flops=10**6, placed=[mine])
    other = lax.ppermute(trunk, "trades_1", [(0, 1), (1, 0)])
    (g_head_all,) = call(
        head_out_kernel, [act], [], [mine], flops=10**8, placed=[mine], final=(0,)
    )
    other, g_head_all = lax.optimization_barrier((other, g_head_all))
    g_in, g_b_in, g_mid, pay6 = call(
        infer_kernel,
        [(64, 512), (1, 512), (512, 512), (32, 1, 128)],
        [core],
        [trunk, other, w_in, w_mid, small, g_b_near, x_infer_t],
        flops=10**9,
        placed=[trunk, other, small, g_b_near],
        scratch=[(64, 512), (1, 512), (512, 512)],
        copies=3,
        final=(0, 1, 2),
    )
    arr6 = swap(pay6, PATHS)
    (exposure,) = call(
        finish_kernel, [(4, 16)], [], [arr6], flops=10**6, placed=[arr6], final=(0,)
    )
    return (g_in, g_b_in.reshape(-1), g_mid, g_b_mid.reshape(-1), g_head_all, exposure)


def solution(mesh):
    torus = Mesh(mesh.devices.reshape(4, 8, 8, 2), PATHS + TRADES)
    return jax.shard_map(
        on_device,
        mesh=torus,
        in_specs=(
            P(PATHS, None),
            P(PATHS, TRADES),
            P(PATHS, None),
            P(None, PATHS, None),
            P(),
            P(),
            P(),
            P(),
            P(None, TRADES),
            P(TRADES),
            P(TRADES),
            P(TRADES),
        ),
        out_specs=(P(), P(), P(), P(), P(None, TRADES), P(None, TRADES)),
        check_vma=False,
    )
```

```python
import functools

import jax
import jax.numpy as jnp
from jax import lax
from jax.experimental import pallas as pl
from jax.experimental.pallas import tpu as pltpu
from jax.sharding import Mesh
from jax.sharding import PartitionSpec as P

TRADES = ("trades_0", "trades_1")
PATHS = ("x", "z")
F32 = jnp.float32
BF16 = jnp.bfloat16

NN = (((1,), (0,)), ((), ()))
NT = (((1,), (1,)), ((), ()))

VALUE_SCALE = 2.0 / (8192 * 4096)
SLOPE_SCALE = 2.0 / (8192 * 64)
PORT_SCALE = 1.0 / 64.0
LEARN = 0.5

LANE_BMID = 96
LANE_BIN = 104
LANE_PORT = 105
LANE_NET = 112
LANE_NET_UPPER = 96
LANE_BIN_LATE = 64


def halves(a):
    high = a.astype(BF16)
    low = (a - high.astype(F32)).astype(BF16)
    return high, low


def mm(left, right, dims=NN):
    def dot(a, b):
        return lax.dot_general(a, b, dims, preferred_element_type=F32)

    return dot(left[0], right[0]) + (dot(left[0], right[1]) + dot(left[1], right[0]))


def mm_narrow(left, right, dims=NN):
    both = jnp.concatenate(right, axis=1 if dims is NN else 0)
    wide = lax.dot_general(left[0], both, dims, preferred_element_type=F32)
    rest = lax.dot_general(left[1], right[0], dims, preferred_element_type=F32)
    return wide[:, 0:128] + (wide[:, 128:256] + rest)


def softplus(z):
    return jnp.maximum(z, 0.0) + jnp.log(1.0 + jnp.exp(-jnp.abs(z)))


def trade_weights(sign, level):
    return (2 * sign - 1).astype(F32) * (0.5 + 0.25 * level.astype(F32))


def column_of(row):
    return jnp.broadcast_to(row, (128, row.shape[1])).T[:, 0:1]


def lane_index(shape):
    return lax.broadcasted_iota(jnp.int32, shape, len(shape) - 1)


def forward_kernel(
    path, trade, core, x_t, w_in, b_in, w_mid, b_mid, head, label, sign, level, sets,
    own, other, a1_t, a2_t, dv_t, small,
):
    first = core[0] == 0
    wt = w_in[...].T
    z1 = mm(halves(wt), halves(x_t[...])) + column_of(b_in[...])
    a1 = softplus(z1)
    a1_t[...] = a1
    mt = w_mid[...].T
    z2 = mm(halves(mt), halves(a1)) + column_of(b_mid[...])
    a2 = softplus(z2)
    a2_t[...] = a2
    hd = head[...]
    values = mm(halves(hd.T), halves(a2))
    err = (values - label[...].T) * VALUE_SCALE
    dv_t[...] = err
    err_p = halves(err)
    d_a2 = mm(halves(hd), err_p)
    w = trade_weights(sign[...], level[...])

    def place(block, rows, start):
        pairs = block.reshape(8, 2, rows, 128)
        even = pairs[:, 0]
        odd = pairs[:, 1]
        own[:, start : start + rows, :] = jnp.where(first, even, odd)
        other[:, start : start + rows, :] = jnp.where(first, odd, even)

    place(d_a2[:, 0:128], 32, 0)
    place(d_a2[:, 128:256], 32, 32)
    small[0:1, 0:256] = w
    small[1:2, 0:256] = sets[...].astype(F32)
    small[2:3, :] = b_in[...]
    small[3:4, :] = b_mid[...]
    port = jnp.sum(hd * w, axis=1, keepdims=True)
    rows = []
    for k in range(4):
        col = jnp.broadcast_to(port[128 * k : 128 * k + 128], (128, 128))
        rows.append(col.T[0:1])
    tile = jnp.concatenate(rows + [jnp.zeros((4, 128), F32)], axis=0)
    own[:, 64:72, :] = jnp.broadcast_to(tile[None], (8, 8, 128))
    other[:, 64:72, :] = jnp.broadcast_to(tile[None], (8, 8, 128))


def join_kernel(own, got, out):
    out[...] = own[...] + got[...]


def head_grad_kernel(a2_t, dv_t, out):
    out[...] = mm(halves(a2_t[...]), halves(dv_t[...]), NT)


def backward_kernel(
    own, arrived, x_t, slope_label_t, w_in, w_mid, a1_t, a2_t, g_head,
    pay, s2_s, u2_s, q_s, z_s,
):
    rows = pl.ds(pl.multiple_of(own[0] * 32, 32), 32)
    total = jnp.sum(arrived[...], axis=0)
    d_a2 = jnp.concatenate([total[0:32], total[32:64]], axis=1)
    port = jnp.concatenate(
        [column_of(total[64 + k : 65 + k]) for k in range(4)], axis=0
    ) * PORT_SCALE
    a1 = a1_t[...]
    a2 = a2_t[...]
    s1 = 1.0 - jnp.exp(-a1)
    s2 = 1.0 - jnp.exp(-a2)
    s2_s[...] = s2
    u2 = port * s2
    u2_s[...] = u2
    mid_p = halves(w_mid[...])
    v1 = mm(mid_p, halves(u2))
    u1 = v1 * s1
    slopes = mm(halves(w_in[...]), halves(u1))
    d_slope = (slopes - slope_label_t[...]) * SLOPE_SCALE
    du1 = mm(halves(w_in[...].T), halves(d_slope))
    dv1 = du1 * s1
    ds1 = du1 * v1
    dv1_p = halves(dv1)
    du2 = mm(halves(w_mid[...].T), dv1_p)
    du2_s2 = du2 * s2
    g_port = jnp.sum(du2_s2, axis=1, keepdims=True)
    q_s[...] = du2_s2 * port * (1.0 - s2)
    dz2 = d_a2 * s2_s[rows, :] + q_s[rows, :]
    z_s[...] = jnp.zeros_like(z_s)
    z_s[rows, :] = dz2
    da1 = mm(mid_p, halves(z_s[...]))
    dz1 = da1 * s1 + (ds1 * s1 * (1.0 - s1)) * (1.0 / 16.0)
    g_b_in = jnp.sum(dz1, axis=1, keepdims=True)
    none = jnp.zeros((64, 256), F32)
    few = jnp.zeros((32, 256), F32)
    mid_a = jnp.concatenate([none, dz2, few], axis=0)
    mid_b = jnp.concatenate([none, u2_s[rows, :], few], axis=0)
    slope_rows = jnp.concatenate([d_slope * (1.0 / 16.0), none], axis=0)
    x_rows = jnp.concatenate([x_t[...], none], axis=0)
    ext = mm_narrow(halves(a1), halves(mid_a), NT)
    ext = ext + mm_narrow(dv1_p, halves(mid_b), NT)
    ext = ext + mm_narrow(halves(u1), halves(slope_rows), NT)
    ext = ext + mm_narrow(halves(dz1), halves(x_rows), NT)
    lane = lane_index((512, 128))
    ext = jnp.where(lane == LANE_BIN, g_b_in, ext)
    ext = jnp.where(lane == LANE_PORT, g_port, ext)
    b_mid = jnp.sum(dz2, axis=1, keepdims=True)
    unit = lax.broadcasted_iota(jnp.int32, (32, 128), 0)
    spot = lane_index((32, 128)) == LANE_BMID + (unit & 7)
    spread = jnp.where(spot, b_mid, 0.0)
    lines = [jnp.sum(spread[8 * k : 8 * k + 8], axis=0, keepdims=True) for k in range(4)]
    tile = jnp.concatenate(lines + [jnp.zeros((4, 128), F32)], axis=0)
    blocks = ext.reshape(64, 8, 128) + tile[None]
    pay[:, 0:8, :] = blocks[0:32]
    pay[:, 8:16, :] = blocks[32:64]
    pay[:, 16:24, :] = g_head[0:256, 0:128].reshape(32, 8, 128)
    pay[:, 24:32, :] = g_head[0:256, 128:256].reshape(32, 8, 128)
    pay[:, 32:40, :] = g_head[256:512, 0:128].reshape(32, 8, 128)
    pay[:, 40:48, :] = g_head[256:512, 128:256].reshape(32, 8, 128)


def net_kernel(own, arrived, head, small, pay, head_shard):
    total = jnp.sum(arrived[...], axis=0)
    trunk = total[0:16]
    w = small[0:1, 0:256]
    upper = jnp.concatenate([total[16:24], total[24:32]], axis=1)
    lower = jnp.concatenate([total[32:40], total[40:48]], axis=1)
    g_head = jnp.concatenate([upper, lower], axis=0)
    g_head = g_head + trunk[:, LANE_PORT : LANE_PORT + 1] * (w * PORT_SCALE)
    head_shard[0:8, :] = g_head[0:8, 0:128]
    head_shard[8:16, :] = g_head[0:8, 128:256]
    head_shard[16:24, :] = g_head[8:16, 0:128]
    head_shard[24:32, :] = g_head[8:16, 128:256]
    first = pl.multiple_of(own[0] * 8, 8)
    second = pl.multiple_of(own[0] * 8 + 256, 8)
    old = jnp.concatenate([head[pl.ds(first, 8), :], head[pl.ds(second, 8), :]], axis=0)
    weighted = halves((old - LEARN * g_head) * w)
    ids = jnp.broadcast_to(small[1:2, 0:256].astype(jnp.int32), (128, 256))
    place = lax.broadcasted_iota(jnp.int32, (128, 256), 0) - LANE_NET
    lane = lane_index((16, 128))
    for t in range(16):
        member = ((ids == place + 16 * t) & (place >= 0)).astype(F32).astype(BF16)
        net = lax.dot_general(weighted[0], member, NT, preferred_element_type=F32)
        net = net + lax.dot_general(weighted[1], member, NT, preferred_element_type=F32)
        pay[t] = jnp.where(lane < LANE_NET, trunk, net)


def gather_kernel(own, arrived, head_shard, pay, g_b_mid, g_b_near):
    total = jnp.sum(arrived[...], axis=0)
    lane = lane_index((16, 128))
    row_lane = lane_index((1, 128))
    first = own[0] == 0
    tiles = []
    for k in range(4):
        block = jnp.zeros((16, 128), F32)
        bias = jnp.zeros((1, 128), F32)
        for m in range(4):
            part = arrived[4 * k + m]
            moved = part if m == 2 else pltpu.roll(part, (32 * m - 64) % 128, 1)
            block = jnp.where((lane >= 32 * m) & (lane < 32 * m + 32), moved, block)
            for r in range(4):
                to = 32 * m + 8 * r
                shift = (to - LANE_BMID) % 128
                line = part[0:8] if shift == 0 else pltpu.roll(part[0:8], shift, 1)
                bias = jnp.where((row_lane >= to) & (row_lane < to + 8), line[r : r + 1], bias)
        g_b_mid[:, 128 * k : 128 * k + 128] = bias
        g_b_near[:, 128 * k : 128 * k + 128] = bias
        tiles.append(jnp.where(first, block[0:8], block[8:16]))
    upper, lower = total[0:8], total[8:16]
    own_rows = jnp.where(first, upper, lower)
    net_shift = (LANE_NET_UPPER - LANE_NET) % 128
    eight = lane_index((8, 128))
    bias_rows = pltpu.roll(own_rows, (LANE_BIN_LATE - LANE_BIN) % 128, 1)
    own_rows = jnp.where(eight < LANE_BIN_LATE, own_rows, bias_rows)
    mixed = jnp.where(eight < LANE_NET_UPPER, own_rows, pltpu.roll(upper, net_shift, 1))
    mixed = jnp.where(eight < LANE_NET, mixed, lower)
    packed = jnp.concatenate(tiles + [mixed, head_shard[...]], axis=0)
    pay[...] = jnp.broadcast_to(packed[None], (8, 72, 128))


def spread_kernel(arrived, out):
    lines = arrived[...].reshape(576, 128)
    out[...] = jnp.broadcast_to(lines[None], (4, 576, 128))


def trim_kernel(arrived, out):
    out[...] = arrived[:, 0:40, :]


def head_out_kernel(arrived, g_head):
    g_head[0:256, 0:128] = arrived[:, 40:48, :].reshape(256, 128)
    g_head[0:256, 128:256] = arrived[:, 48:56, :].reshape(256, 128)
    g_head[256:512, 0:128] = arrived[:, 56:64, :].reshape(256, 128)
    g_head[256:512, 128:256] = arrived[:, 64:72, :].reshape(256, 128)


def infer_kernel(
    own, mine, other, w_in, w_mid, small, g_b_mid, x_t,
    g_in_out, g_b_in_out, g_mid_out, pay, g_in_s, g_b_in_s, g_mid_s, sems,
):
    first = own[0] == 0
    for k in range(4):
        a = mine[:, 8 * k : 8 * k + 8, :].reshape(256, 128)
        b = other[:, 8 * k : 8 * k + 8, :].reshape(256, 128)
        g_mid_s[0:256, 128 * k : 128 * k + 128] = jnp.where(first, a, b)
        g_mid_s[256:512, 128 * k : 128 * k + 128] = jnp.where(first, b, a)
    near = mine[:, 32:40, :].reshape(256, 128)
    away = other[:, 32:40, :].reshape(256, 128)
    upper = jnp.where(first, near, away)
    lower = jnp.where(first, away, near)
    flat = jnp.concatenate([upper, lower], axis=0).T
    g_in = flat[0:64]
    g_b_in = flat[LANE_BIN_LATE : LANE_BIN_LATE + 1]
    net_shift = (LANE_NET - LANE_NET_UPPER) % 128
    both = jnp.concatenate([pltpu.roll(near, net_shift, 1), near], axis=0)
    g_in_s[...] = g_in
    g_b_in_s[...] = g_b_in
    copies = [
        pltpu.make_async_copy(g_mid_s, g_mid_out, sems.at[0]),
        pltpu.make_async_copy(g_in_s, g_in_out, sems.at[1]),
        pltpu.make_async_copy(g_b_in_s, g_b_in_out, sems.at[2]),
    ]
    for copy in copies:
        copy.start()
    new_in = halves(w_in[...] - LEARN * g_in)
    deep_in = jnp.concatenate([new_in[0], new_in[0], new_in[1]], axis=0)
    new_b_in = small[2:3, :] - LEARN * g_b_in
    new_mid = halves(w_mid[...] - LEARN * g_mid_s[...])
    new_b_mid = small[3:4, :] - LEARN * g_b_mid[...]
    net_head = halves(both)
    row = jnp.zeros((1, 128), F32)
    lane = lane_index((1, 128))
    x_rows = jnp.concatenate([x_t[d].T for d in range(4)], axis=0)
    high, low = halves(x_rows)
    first_pre = jnp.dot(
        jnp.concatenate([high, low, high], axis=1), deep_in, preferred_element_type=F32
    )
    a1 = softplus(first_pre + new_b_in)
    a2 = softplus(mm(halves(a1), new_mid) + new_b_mid)
    netted = jnp.maximum(mm_narrow(halves(a2), net_head), 0.0)
    for d in range(4):
        line = jnp.sum(netted[256 * d : 256 * d + 256], axis=0, keepdims=True)
        moved = pltpu.roll(line, (16 * d - LANE_NET) % 128, 1)
        row = jnp.where((lane >= 16 * d) & (lane < 16 * d + 16), moved, row)
    pay[...] = jnp.broadcast_to(row[None], (32, 1, 128))
    for copy in copies:
        copy.wait()


def finish_kernel(lines, exposure):
    total = jnp.sum(lines[...], axis=0) * (1.0 / 8192.0)
    for d in range(4):
        moved = total if d == 0 else pltpu.roll(total, 128 - 16 * d, 1)
        exposure[d : d + 1, :] = moved[:, 0:16]


def keep(a):
    return pltpu.with_memory_space_constraint(a, pltpu.VMEM)


def far(a):
    return pltpu.with_memory_space_constraint(a, pltpu.HBM)


def call(kernel, outs, scalars, args, scratch=(), flops=0, placed=(), final=(), away=(), copies=0):
    shapes = tuple(
        pltpu.HBM(s, F32) if i in final else pltpu.VMEM(s, F32)
        for i, s in enumerate(outs)
    )
    semaphores = [pltpu.SemaphoreType.DMA((copies,))] if copies else []
    vmem = pl.BlockSpec(memory_space=pltpu.VMEM)
    smem = pl.BlockSpec(memory_space=pltpu.SMEM)
    args = [keep(a) if any(a is p for p in placed) else a for a in args]
    args = [far(a) if any(a is p for p in away) else a for a in args]
    return pl.pallas_call(
        kernel,
        out_shape=shapes,
        in_specs=[smem] * len(scalars) + [vmem] * len(args),
        out_specs=tuple(
            pl.BlockSpec(memory_space=pl.ANY) if i < copies else vmem for i in range(len(outs))
        ),
        scratch_shapes=[pltpu.VMEM(s, F32) for s in scratch] + semaphores,
        cost_estimate=pl.CostEstimate(flops=flops, transcendentals=0, bytes_accessed=0),
        compiler_params=pltpu.CompilerParams(vmem_limit_bytes=24 * 2**20),
        name=kernel.__name__,
    )(*scalars, *args)


def swap(x, axis):
    return lax.all_to_all(x, axis, 0, 0, tiled=True)


def on_device(
    x_train, value_label, slope_label, x_infer, w_in, b_in, w_mid, b_mid, head,
    trade_set, trade_sign, trade_level,
):
    path = lax.axis_index(PATHS).astype(jnp.int32).reshape(1)
    trade = lax.axis_index(TRADES).astype(jnp.int32).reshape(1)
    core = lax.axis_index("trades_1").astype(jnp.int32).reshape(1)
    b_in_r = b_in.reshape(1, -1)
    b_mid_r = b_mid.reshape(1, -1)
    sets = trade_set.reshape(1, -1)
    sign = trade_sign.reshape(1, -1)
    level = trade_level.reshape(1, -1)
    act = (512, 256)
    x_t = x_train.T
    slope_label_t = slope_label.T
    x_infer_t = x_infer.transpose(0, 2, 1)
    own, other, a1_t, a2_t, dv_t, small = call(
        forward_kernel,
        [(8, 72, 128), (8, 72, 128), act, act, (256, 256), (8, 512)],
        [path, trade, core],
        [x_t, w_in, b_in_r, w_mid, b_mid_r, head, value_label, sign, level, sets],
        flops=10**9,
        away=[x_t, w_in, w_mid, head, value_label, b_in_r, b_mid_r, sign, level, sets],
    )
    got = lax.ppermute(other, "trades_1", [(0, 1), (1, 0)])
    (g_head,) = call(
        head_grad_kernel,
        [act],
        [],
        [a2_t, dv_t],
        flops=4 * 10**8,
        placed=[a2_t, dv_t],
    )
    (pay1,) = call(join_kernel, [(8, 72, 128)], [], [own, got], flops=10**6, placed=[own, got])
    pay1, g_head = lax.optimization_barrier((pay1, g_head))
    arr1 = swap(pay1, "trades_0")
    (pay2,) = call(
        backward_kernel,
        [(32, 48, 128)],
        [trade],
        [arr1, x_t, slope_label_t, w_in, w_mid, a1_t, a2_t, g_head],
        scratch=[act, act, act, act],
        flops=10**9,
        placed=[arr1, w_mid, a1_t, a2_t, g_head, x_t, slope_label_t, w_in],
    )
    arr2 = swap(pay2, PATHS)
    pay3, head_shard = call(
        net_kernel,
        [(16, 16, 128), (32, 128)],
        [path],
        [arr2, head, small],
        flops=10**8,
        placed=[arr2, small],
    )
    arr3 = swap(pay3, TRADES)
    pay4, g_b_mid, g_b_near = call(
        gather_kernel,
        [(8, 72, 128), (1, 512), (1, 512)],
        [core],
        [arr3, head_shard],
        flops=10**8,
        placed=[arr3, head_shard],
        final=(1,),
    )
    arr4 = swap(pay4, "z")
    (pay5,) = call(spread_kernel, [(4, 576, 128)], [], [arr4], flops=10**6, placed=[arr4])
    mine = swap(pay5, "x").reshape(32, 72, 128)
    (trunk,) = call(trim_kernel, [(32, 40, 128)], [], [mine], flops=10**6, placed=[mine])
    other = lax.ppermute(trunk, "trades_1", [(0, 1), (1, 0)])
    (g_head_all,) = call(
        head_out_kernel, [act], [], [mine], flops=10**8, placed=[mine], final=(0,)
    )
    other, g_head_all = lax.optimization_barrier((other, g_head_all))
    g_in, g_b_in, g_mid, pay6 = call(
        infer_kernel,
        [(64, 512), (1, 512), (512, 512), (32, 1, 128)],
        [core],
        [trunk, other, w_in, w_mid, small, g_b_near, x_infer_t],
        flops=10**9,
        placed=[trunk, other, small, g_b_near],
        scratch=[(64, 512), (1, 512), (512, 512)],
        copies=3,
        final=(0, 1, 2),
    )
    arr6 = swap(pay6, PATHS)
    (exposure,) = call(
        finish_kernel, [(4, 16)], [], [arr6], flops=10**6, placed=[arr6], final=(0,)
    )
    return (g_in, g_b_in.reshape(-1), g_mid, g_b_mid.reshape(-1), g_head_all, exposure)


def solution(mesh):
    torus = Mesh(mesh.devices.reshape(4, 8, 8, 2), PATHS + TRADES)
    return jax.shard_map(
        on_device,
        mesh=torus,
        in_specs=(
            P(PATHS, None),
            P(PATHS, TRADES),
            P(PATHS, None),
            P(None, PATHS, None),
            P(),
            P(),
            P(),
            P(),
            P(None, TRADES),
            P(TRADES),
            P(TRADES),
            P(TRADES),
        ),
        out_specs=(P(), P(), P(), P(), P(None, TRADES), P(None, TRADES)),
        check_vma=False,
    )
```
